512 devices in a mesh: member: 16 (over z, y_hi), dp: 32 (over y_lo, x, core).
Axes of the slice: x: 4, y: 8 (y_hi: 2, y_lo: 4; y = y_hi * 4 + y_lo), z: 8, core: 2. Of those that a mesh axis runs over, the one named last changes fastest.
Arguments:
- teacher_feats: bfloat16 [16, 512, 1024], P('member', 'dp'), may hold values from -8 to 8
- teacher_gain: float32 [16, 1024], P('member'), may hold values from 0.1 to 1.9
- teacher_head: bfloat16 [16, 1024, 12288], P('member', None, 'dp'), may hold values from -1 to 1
- teacher_bias: float32 [16, 12288], P('member', 'dp'), may hold values from -1 to 4
- student_feats: bfloat16 [512, 1024], P('member'), may hold values from -6 to 6
- student_gain: float32 [1024], replicated, may hold values from 0.1 to 1.9
- student_head: bfloat16 [1024, 12288], P('member', 'dp'), may hold values from -0.1875 to 0.1875
- student_bias: float32 [12288], P('dp'), may hold values from -1 to 4
Outputs:
- loss: float32 [], replicated
- head_grad: float32 [1024, 12288], P('member', 'dp')
- bias_grad: float32 [12288], P('dp')
The draws below stay inside these ranges and needn't reach their ends.
All inputs are finite; a program needn't handle non-finite values.
Results may differ from the reference program's by a relative error of at most 0.022.
Values may be sent and summed in bfloat16 or wider, within the bound.
A program may use at most 64 MiB of HBM per device.

```python
import math
import jax
import jax.numpy as jnp
from jax import lax

D = 1024
MEMBERS = 16
IMAGES = 512
CLASSES = 12288


def teacher_pair(key):
    base_key = jax.random.fold_in(key, 7101)
    subkeys = jax.random.split(base_key, 2)
    features = jax.random.normal(subkeys[0], (MEMBERS, IMAGES, D), jnp.float32)
    weights = jnp.clip(jax.random.normal(subkeys[1], (MEMBERS, D, CLASSES), jnp.float32), -5.0, 5.0) * (3.0 / math.sqrt(D))
    features = jnp.clip(features, -6.0, 6.0)
    return (features, weights)


def rising_offsets(key, salt, shape):
    sub_key = jax.random.fold_in(key, salt)
    position = lax.broadcasted_iota(jnp.float32, shape, len(shape) - 1) / CLASSES
    return jax.random.uniform(sub_key, shape, jnp.float32, -1.0, 1.0) + 1.1 * position


def draw_teacher_feats(key, part):
    return teacher_pair(key)[0].astype(jnp.bfloat16)


def draw_teacher_head(key, part):
    return teacher_pair(key)[1].astype(jnp.bfloat16)


def draw_teacher_bias(key, part):
    return rising_offsets(key, 7202, (MEMBERS, CLASSES))


def draw_student_bias(key, part):
    return rising_offsets(key, 7303, (CLASSES,))


def strengthened(entries, rng, source, target, parts, factor):
    owner, partner = [(jnp.arange(entries.shape[dim]) // (entries.shape[dim] // parts)).reshape([-1 if axis == dim else 1 for axis in range(entries.ndim)]) for dim in (source, target)]
    chosen = jax.random.permutation(rng, parts)[partner]
    strong = (owner == chosen) | (owner == (partner + parts // 2) % parts)
    return jnp.where(strong, factor * entries, entries)


def level_of(rng, extent, shards, smallest, largest):
    def one(dim, parts):
        draws = jax.random.uniform(jax.random.fold_in(jax.random.fold_in(rng, 6), dim), (parts,), jnp.float32, smallest / len(shards), largest / len(shards))
        return jnp.repeat(jnp.exp(draws), extent[dim] // parts).reshape((-1,) + (1,) * (len(extent) - dim - 1))

    level = one(*shards[0])
    for cut in shards[1:]:
        level = level * one(*cut)
    return level


def scatter_about(own_key, shape, width, bound, shards=(), held_as=jnp.bfloat16):
    entries = width * jax.random.normal(own_key, shape, jnp.float32)
    if shards:
        entries = entries * level_of(own_key, shape, shards, -0.22, 0.18)
    return jnp.clip(entries, -bound, bound).astype(held_as)


def heavy_noise(rng, extent, scale, reach, cuts, heavy, dtype=jnp.bfloat16):
    result = scale * jax.random.normal(rng, extent, jnp.float32)
    if cuts:
        result = result * level_of(rng, extent, cuts, -0.22, 0.18)
    return jnp.clip(strengthened(result, jax.random.fold_in(rng, 3), *heavy), -reach, reach).astype(dtype)


def setup_inputs(seed: int = 0) -> dict:
    splits = jax.random.split(jax.random.key(seed), 9)
    teacher_feats = draw_teacher_feats(jax.random.fold_in(splits[8], 71), 0)
    teacher_gain = jnp.clip(1.0 + 0.18 * jax.random.normal(splits[1], (MEMBERS, D), jnp.float32), 0.1, 1.9)
    teacher_head = draw_teacher_head(jax.random.fold_in(splits[8], 71), 0)
    teacher_bias = draw_teacher_bias(jax.random.fold_in(splits[8], 71), 0)
    student_feats = heavy_noise(splits[4], (IMAGES, D), 1.0, 6.0, ((0, 16),), (0, 1, 16, 2.0))
    student_gain = jnp.clip(1.0 + 0.18 * jax.random.normal(splits[5], (D,), jnp.float32), 0.1, 1.9)
    student_head = scatter_about(splits[6], (D, CLASSES), D ** -0.5, 0.1875, ((0, 16), (1, 32)))
    student_bias = draw_student_bias(jax.random.fold_in(splits[8], 71), 0)
    return dict(teacher_feats=teacher_feats, teacher_gain=teacher_gain, teacher_head=teacher_head, teacher_bias=teacher_bias, student_feats=student_feats, student_gain=student_gain, student_head=student_head, student_bias=student_bias)


def norm_rows(values, gain_row):
    values = values.astype(jnp.float32)
    center = values - lax.optimization_barrier(jnp.mean(values, axis=-1, keepdims=True))
    spread = lax.optimization_barrier(jnp.mean(center * center, axis=-1, keepdims=True))
    return center * lax.rsqrt(spread + 1e-06) * gain_row

def reference(teacher_feats, teacher_gain, teacher_head, teacher_bias, student_feats, student_gain, student_head, student_bias):
    members = teacher_feats.shape[0]
    images = teacher_feats.shape[1]

    def member_step(running, inputs):
        features, gain_row, weights, offsets = inputs
        normed = norm_rows(features, gain_row).astype(jnp.bfloat16)
        logits = jnp.dot(normed, weights, preferred_element_type=jnp.float32) + offsets
        maxima = lax.optimization_barrier(jnp.max(logits, axis=1, keepdims=True))
        log_norm = maxima + jnp.log(lax.optimization_barrier(jnp.sum(jnp.exp(logits - maxima), axis=1, keepdims=True)))
        rounded = lax.optimization_barrier((logits - log_norm).astype(jnp.bfloat16))
        return (running + rounded.astype(jnp.float32), None)
    summed, _ = lax.scan(member_step, jnp.zeros((images, CLASSES), jnp.float32), (teacher_feats, teacher_gain, teacher_head, teacher_bias))
    target = summed / members
    normed_s = norm_rows(student_feats, student_gain).astype(jnp.bfloat16)
    alphas = jnp.exp(jnp.dot(normed_s, student_head, preferred_element_type=jnp.float32) + student_bias)
    alpha_sum = lax.optimization_barrier(jnp.sum(alphas, axis=1, keepdims=True))
    per_image = -lax.lgamma(alpha_sum[:, 0]) + lax.optimization_barrier(jnp.sum(lax.lgamma(alphas) - (alphas - 1.0) * target, axis=1))
    loss_value = jnp.sum(per_image) / (images * CLASSES)
    signal = alphas * (lax.digamma(alphas) - lax.digamma(alpha_sum) - target)
    head_grad = lax.dot_general(normed_s.astype(jnp.float32), signal, (((0,), (0,)), ((), ())), precision=lax.Precision.HIGHEST, preferred_element_type=jnp.float32) / images
    bias_grad = lax.optimization_barrier(jnp.sum(signal, axis=0)) / images
    return (loss_value, head_grad, bias_grad)
```

```python
import functools

import jax
import jax.numpy as jnp
from jax import lax
from jax.experimental import pallas as pl
from jax.experimental.pallas import tpu as pltpu
from jax.sharding import Mesh
from jax.sharding import PartitionSpec as P

MEMBER = ("member_0", "member_1")
DP = ("dp_0", "dp_1", "dp_2")
AXES = MEMBER + DP
LANES = 128
F32 = jnp.float32
BF16 = jnp.bfloat16
NT = (((1,), (1,)), ((), ()))


def norm_rows(values, gain_row):
    values = values.astype(F32)
    center = values - jnp.mean(values, axis=-1, keepdims=True)
    spread = jnp.mean(center * center, axis=-1, keepdims=True)
    return center * lax.rsqrt(spread + 1e-06) * gain_row


def gamma_parts(x):
    small = x < 8.0
    base = jnp.where(small, x, 1.0)
    product = base
    harmonic = 1.0 / base
    for step in range(1, 8):
        product = product * (base + step)
        harmonic = harmonic + 1.0 / (base + step)
    big = jnp.where(small, x + 8.0, x)
    log_big = jnp.log(big)
    inv = 1.0 / big
    inv2 = inv * inv
    lgamma = (big - 0.5) * log_big - big + 0.9189385332046727
    lgamma = lgamma + inv * (1.0 / 12 - inv2 * (1.0 / 360 - inv2 * (1.0 / 1260)))
    digamma = log_big - 0.5 * inv - inv2 * (1.0 / 12 - inv2 * (1.0 / 120 - inv2 * (1.0 / 252)))
    lgamma = lgamma - jnp.where(small, jnp.log(product), 0.0)
    digamma = digamma - jnp.where(small, harmonic, 0.0)
    return lgamma, digamma


def start_copy(src, dst, send_sem, recv_sem, device):
    pltpu.make_async_remote_copy(
        src_ref=src,
        dst_ref=dst,
        send_sem=send_sem,
        recv_sem=recv_sem,
        device_id=device,
        device_id_type=pl.DeviceIdType.MESH,
    ).start()


def wait_bytes(ref, sem):
    pltpu.make_async_copy(ref, ref, sem).wait()


def step_kernel(
    sizes,
    tf_h, tg_h, w_h, tb_h, sf_h, sg_h, sh_h, sb_h,
    hg_o, bias_o, loss_o,
    tfv, tgv, wv, tbv, sfv, sgv, sbv,
    xn, wt, tbt, lg, send, rb, tz, tb_s, tp,
    bm, bs, st, vs, vr, vz, vp,
    sn, shb, sws, swr, sbt, ad, asum, az, al_s,
    bc, bg_s, bgr, bh, bp, hs, hr, ht, hb, hp,
    ld, l_s, lz, lh, lp,
    in_sems, xn_sems, sn_sems, rb_sems, one, out,
):
    Z, H, Y, X, C = sizes
    z, h, y, x, c = (lax.axis_index(a) for a in AXES)
    dpn = Y * X * C
    me = (y * X + x) * C + c
    D = xn.shape[2]
    rows_t = xn.shape[1]
    L = wt.shape[0]
    cb = L // Z
    half_blocks = dpn // H
    ih = half_blocks * rows_t
    rows_s = ih // Z
    q = rows_s // rows_t
    images = ih * H

    def at(nz=None, nh=None, ny=None, nx=None, nc=None):
        new = (nz, nh, ny, nx, nc)
        return tuple(old if n is None else n for old, n in zip((z, h, y, x, c), new))

    def spot(py, px, pc):
        d = (py * X + px) * C + pc
        m = d // q
        return (m % H) * half_blocks + (m // H) * q + d % q

    def ring(k):
        return lax.rem(z + k, Z)

    z_order = sorted(range(1, Z), key=lambda k: -min(k, Z - k))
    plane = [
        (lax.rem(y + i, Y), lax.rem(x + j, X), lax.rem(c + k, C))
        for i in reversed(range(Y))
        for j in range(X)
        for k in range(C)
        if i or j or k
    ]

    loads = [
        pltpu.make_async_copy(src, dst, in_sems.at[i])
        for i, (src, dst) in enumerate(
            [
                (tf_h.at[0], tfv),
                (tg_h, tgv),
                (sf_h, sfv),
                (sg_h, sgv),
                (sh_h, shb.at[h]),
                (tb_h, tbv),
                (sb_h, sbv),
                (w_h.at[0], wv),
            ]
        )
    ]
    for load in loads:
        load.start()
    barrier = pltpu.get_barrier_semaphore()
    peers = [at(ny=a, nx=b, nc=e) for a, b, e in plane]
    peers += [at(nz=ring(k)) for k in range(1, Z)] + [at(nh=1 - h)]
    for peer in peers:
        pl.semaphore_signal(barrier, 1, device_id=peer, device_id_type=pl.DeviceIdType.MESH)

    own = spot(y, x, c)
    loads[0].wait()
    loads[1].wait()
    xn[own] = norm_rows(tfv[...], tgv[...]).astype(BF16)
    loads[2].wait()
    loads[3].wait()
    sn[pl.ds(z * C, C)] = norm_rows(sfv[...], sgv[...]).astype(BF16).reshape(C, rows_s // C, D)
    loads[4].wait()
    pl.semaphore_wait(barrier, len(peers))

    def forward(block, device):
        start_copy(xn.at[block], xn.at[block], out.at[0], xn_sems.at[block], device)

    for k in reversed(range(1, Y)):
        forward(own, at(ny=lax.rem(y + k, Y)))
    for j in range(1, X):
        forward(own, at(nx=lax.rem(x + j, X)))
    for e in range(1, C):
        forward(own, at(nc=lax.rem(c + e, C)))
    start_copy(shb.at[h], shb.at[h], out.at[1], one.at[0], at(nh=1 - h))
    mine = z * C + c
    for k in z_order:
        start_copy(sn.at[mine], sn.at[mine], out.at[2], sn_sems.at[mine], at(nz=ring(k)))

    loads[5].wait()
    loads[6].wait()
    tbt[...] = jnp.broadcast_to(tbv[...], (LANES, L)).T
    sbt[...] = jnp.broadcast_to(sbv[...], (LANES, L)).T
    loads[7].wait()
    for k in range(D // LANES):
        part = slice(k * LANES, (k + 1) * LANES)
        wt[:, part] = wv[part, :].astype(F32).T.astype(BF16)

    for k in range(1, Y):
        py = lax.rem(y + k, Y)
        block = spot(py, x, c)
        wait_bytes(xn.at[block], xn_sems.at[block])
        for j in range(1, X):
            forward(block, at(nx=lax.rem(x + j, X)))
        for e in range(1, C):
            forward(block, at(nc=lax.rem(c + e, C)))

    wait_bytes(shb.at[1 - h], one.at[0])
    turned = shb[...].astype(F32).reshape(shb.shape[0] * shb.shape[1], L).T
    sws[...] = turned.astype(BF16).reshape(Z, cb, LANES)
    for k in z_order:
        start_copy(sws.at[ring(k)], swr.at[z], out.at[3], one.at[1], at(nz=ring(k)))
    swr[z] = sws[z]

    for j in range(1, X):
        px = lax.rem(x + j, X)
        for k in range(Y):
            block = spot(lax.rem(y + k, Y), px, c)
            wait_bytes(xn.at[block], xn_sems.at[block])
            for e in range(1, C):
                forward(block, at(nc=lax.rem(c + e, C)))
    for k in range(1, Z):
        block = ring(k) * C + c
        wait_bytes(sn.at[block], sn_sems.at[block])
        for e in range(1, C):
            start_copy(
                sn.at[block], sn.at[block], out.at[2], sn_sems.at[block], at(nc=lax.rem(c + e, C))
            )
    for e in range(1, C):
        pc = lax.rem(c + e, C)
        for k in range(Y):
            for j in range(X):
                block = spot(lax.rem(y + k, Y), lax.rem(x + j, X), pc)
                wait_bytes(xn.at[block], xn_sems.at[block])

    for a in range(H):
        held = xn[a * half_blocks : (a + 1) * half_blocks].reshape(ih, D)
        lg[a] = lax.dot_general(wt[...], held, NT, preferred_element_type=F32)
    for k in z_order + [0]:
        to = ring(k)
        rows = pl.ds(pl.multiple_of(to * cb, 16), cb)
        part = lg[:, rows, :] + tbt[rows, 0:1][None]
        top = jnp.max(part, axis=1, keepdims=True)
        part = part - top
        send[to] = part.astype(BF16)
        bm[to] = top
        bs[to] = jnp.sum(jnp.exp(part), axis=1, keepdims=True)
        if k:
            start_copy(send.at[to], rb.at[z], out.at[4], rb_sems.at[z], at(nz=to))
    tops = bm[...]
    top = jnp.max(tops, axis=0)
    st[me] = top + jnp.log(jnp.sum(bs[...] * jnp.exp(tops - top[None]), axis=0))
    for a, b, e in plane:
        start_copy(st.at[me], st.at[me], out.at[5], one.at[2], at(ny=a, nx=b, nc=e))

    for e in range(1, C):
        pc = lax.rem(c + e, C)
        for k in range(1, Z):
            block = ring(k) * C + pc
            wait_bytes(sn.at[block], sn_sems.at[block])
    wait_bytes(swr.at[pl.ds(0, Z - 1)], one.at[1])
    scores = jnp.zeros((cb, ih), F32)
    for k in range(Z):
        part = slice(k * LANES, (k + 1) * LANES)
        scores = scores + lax.dot_general(
            swr[k], sn[:, :, part].reshape(ih, LANES), NT, preferred_element_type=F32
        )
    my_rows = pl.ds(pl.multiple_of(z * cb, 16), cb)
    alphas = jnp.exp(scores + sbt[my_rows, 0:1])
    al_s[...] = alphas
    ad[me] = jnp.sum(alphas, axis=0, keepdims=True)
    for a, b, e in plane:
        start_copy(ad.at[me], ad.at[me], out.at[6], one.at[3], at(ny=a, nx=b, nc=e))

    wait_bytes(st.at[pl.ds(0, dpn - 1)], one.at[2])
    tops = st[...]
    top = jnp.max(tops, axis=0)
    log_norm = top + jnp.log(jnp.sum(jnp.exp(tops - top[None]), axis=0))
    vs[...] = bm[...] - log_norm[None]
    for k in z_order:
        start_copy(vs.at[ring(k)], vr.at[z], out.at[7], one.at[4], at(nz=ring(k)))
    vr[z] = vs[z]

    wait_bytes(ad.at[pl.ds(0, dpn - 1)], one.at[3])
    asum[...] = jnp.sum(ad[...], axis=0)
    for k in z_order:
        start_copy(asum, az.at[z], out.at[8], one.at[5], at(nz=ring(k)))
    az[z] = asum[...]
    lgamma, digamma = gamma_parts(al_s[...])

    total = send[z].astype(F32)
    for k in range(1, Z):
        wait_bytes(rb.at[ring(k)], rb_sems.at[ring(k)])
        total = total + rb[ring(k)].astype(F32)
    tz[...] = total
    tb_s[...] = tz[1 - h].astype(BF16)
    start_copy(tb_s, tp, out.at[9], one.at[6], at(nh=1 - h))
    wait_bytes(vr.at[pl.ds(0, Z - 1)], one.at[4])
    vz[...] = jnp.sum(vr[...], axis=0)
    start_copy(vz.at[1 - h], vp, out.at[10], one.at[7], at(nh=1 - h))
    wait_bytes(az.at[pl.ds(0, Z - 1)], one.at[5])
    lgamma_sum, digamma_sum = gamma_parts(jnp.sum(az[...], axis=0))
    wait_bytes(vp, one.at[7])
    shift = vz[h] + vp[...]
    wait_bytes(tp, one.at[6])
    target = (tz[h] + tp[...].astype(F32) + shift) / (Z * H)

    alphas = al_s[...]
    signal = alphas * (digamma - digamma_sum - target)
    terms = jnp.sum(lgamma - (alphas - 1.0) * target, axis=0, keepdims=True)
    terms = terms - lgamma_sum / (Z * dpn)
    ld[me] = jnp.broadcast_to(jnp.sum(terms, axis=1, keepdims=True), (1, LANES))
    for a, b, e in plane:
        start_copy(ld.at[me], ld.at[me], out.at[11], one.at[8], at(ny=a, nx=b, nc=e))

    high = signal.astype(BF16)
    rest = signal - high.astype(F32)
    mid = rest.astype(BF16)
    low = (rest - mid.astype(F32)).astype(BF16)
    parts = lax.dot_general(
        jnp.concatenate([high, mid, low], axis=0),
        sn[...].reshape(ih, D),
        (((1,), (0,)), ((), ())),
        preferred_element_type=F32,
    )
    grad = parts[:cb] + parts[cb : 2 * cb] + parts[2 * cb :]
    for k in range(Z):
        hs[k] = grad[:, k * LANES : (k + 1) * LANES].astype(BF16)
    for k in z_order:
        start_copy(hs.at[ring(k)], hr.at[z], out.at[12], one.at[9], at(nz=ring(k)))
    hr[z] = hs[z]
    bc[...] = jnp.zeros_like(bc)
    bc[my_rows, :] = jnp.broadcast_to(jnp.sum(signal, axis=1, keepdims=True), (cb, LANES))
    bg_s[...] = bc[...].T[0:1]
    for k in z_order:
        start_copy(bg_s, bgr.at[z], out.at[13], one.at[10], at(nz=ring(k)))
    bgr[z] = bg_s[...]

    wait_bytes(ld.at[pl.ds(0, dpn - 1)], one.at[8])
    l_s[...] = jnp.sum(ld[...], axis=0)
    for k in z_order:
        start_copy(l_s, lz.at[z], out.at[14], one.at[11], at(nz=ring(k)))
    lz[z] = l_s[...]

    wait_bytes(hr.at[pl.ds(0, Z - 1)], one.at[9])
    rows = hr[...].astype(F32).reshape(L, LANES).T
    ht[...] = rows.reshape(H, LANES // H, L)
    hb[...] = ht[1 - h].astype(BF16)
    start_copy(hb, hp, out.at[15], one.at[12], at(nh=1 - h))
    wait_bytes(bgr.at[pl.ds(0, Z - 1)], one.at[10])
    bh[...] = jnp.sum(bgr[...], axis=0)
    start_copy(bh, bp, out.at[16], one.at[13], at(nh=1 - h))
    wait_bytes(lz.at[pl.ds(0, Z - 1)], one.at[11])
    lh[...] = jnp.sum(lz[...], axis=0)
    start_copy(lh, lp, out.at[17], one.at[14], at(nh=1 - h))

    wait_bytes(bp, one.at[13])
    bias_o[...] = (bh[...] + bp[...]) / images
    wait_bytes(lp, one.at[14])
    loss_o[...] = (lh[...] + lp[...]) / (images * (L * dpn))
    wait_bytes(hp, one.at[12])
    hg_o[...] = (ht[h] + hp[...].astype(F32)) / images

    sent = [
        xn.at[pl.ds(0, dpn - 1)],
        shb.at[h],
        sn.at[pl.ds(0, (Z - 1) * C)],
        sws.at[pl.ds(0, Z - 1)],
        send.at[pl.ds(0, Z - 1)],
        st.at[pl.ds(0, dpn - 1)],
        ad.at[pl.ds(0, dpn - 1)],
        vs.at[pl.ds(0, Z - 1)],
        az.at[pl.ds(0, Z - 1)],
        tb_s,
        vp,
        ld.at[pl.ds(0, dpn - 1)],
        hs.at[pl.ds(0, Z - 1)],
        bgr.at[pl.ds(0, Z - 1)],
        lz.at[pl.ds(0, Z - 1)],
        hb,
        bh,
        lh,
    ]
    for i, ref in enumerate(sent):
        wait_bytes(ref, out.at[i])


def on_device(sizes, tf, tg, w, tb, sf, sg, sh, sb):
    Z, H, Y, X, C = sizes
    dpn = Y * X * C
    rows_t, D = tf.shape[1:]
    L = w.shape[2]
    cb = L // Z
    ih = rows_t * dpn // H
    rows_s = sf.shape[0]
    assert D == Z * LANES and rows_s * Z == ih and sh.shape[0] * H == LANES

    def v(shape, dtype=F32):
        return pltpu.VMEM(shape, dtype)

    scratch = [
        v((rows_t, D), BF16), v((1, D)), v((D, L), BF16), v((1, L)),
        v((rows_s, D), BF16), v((1, D)), v((1, L)),
        v((dpn, rows_t, D), BF16), v((L, D), BF16), v((L, LANES)), v((H, L, ih)),
        v((Z, H, cb, ih), BF16), v((Z, H, cb, ih), BF16), v((H, cb, ih)), v((cb, ih), BF16), v((cb, ih), BF16),
        v((Z, H, 1, ih)), v((Z, H, 1, ih)), v((dpn, H, 1, ih)), v((Z, H, 1, ih)), v((Z, H, 1, ih)),
        v((H, 1, ih)), v((1, ih)),
        v((Z * C, rows_s // C, D), BF16), v((H, LANES // H, L), BF16), v((Z, cb, LANES), BF16),
        v((Z, cb, LANES), BF16), v((L, LANES)), v((dpn, 1, ih)), v((1, ih)), v((Z, 1, ih)), v((cb, ih)),
        v((L, LANES)), v((1, L)), v((Z, 1, L)), v((1, L)), v((1, L)),
        v((Z, cb, LANES), BF16), v((Z, cb, LANES), BF16), v((H, LANES // H, L)),
        v((LANES // H, L), BF16), v((LANES // H, L), BF16),
        v((dpn, 1, LANES)), v((1, LANES)), v((Z, 1, LANES)), v((1, LANES)), v((1, LANES)),
        pltpu.SemaphoreType.DMA((8,)), pltpu.SemaphoreType.DMA((dpn,)), pltpu.SemaphoreType.DMA((Z * C,)),
        pltpu.SemaphoreType.DMA((Z,)), pltpu.SemaphoreType.DMA((15,)), pltpu.SemaphoreType.DMA((18,)),
    ]
    vmem = pl.BlockSpec(memory_space=pltpu.VMEM)
    head_grad, bias_grad, loss = pl.pallas_call(
        functools.partial(step_kernel, sizes),
        out_shape=(
            jax.ShapeDtypeStruct((LANES // H, L), F32),
            jax.ShapeDtypeStruct((1, L), F32),
            jax.ShapeDtypeStruct((1, LANES), F32),
        ),
        in_specs=[pl.BlockSpec(memory_space=pl.ANY)] * 8,
        out_specs=(vmem, vmem, vmem),
        scratch_shapes=scratch,
        compiler_params=pltpu.CompilerParams(
            collective_id=0, has_side_effects=True, vmem_limit_bytes=67043328
        ),
    )(tf, tg, w, tb, sf, sg.reshape(1, -1), sh, sb.reshape(1, -1))
    return loss[0, 0], head_grad, bias_grad[0]


def solution(mesh, sizes=(8, 2, 4, 4, 2)):
    torus = Mesh(mesh.devices.reshape(sizes), AXES)
    placed = (
        P(MEMBER, DP, None),
        P(MEMBER, None),
        P(MEMBER, None, DP),
        P(MEMBER, DP),
        P(MEMBER, None),
        P(),
        P(MEMBER, DP),
        P(DP),
    )
    return jax.shard_map(
        functools.partial(on_device, sizes),
        mesh=torus,
        in_specs=placed,
        out_specs=(P(), P(MEMBER, DP), P(DP)),
        check_vma=False,
    )
```

```python
import functools

import jax
import jax.numpy as jnp
from jax import lax
from jax.experimental import pallas as pl
from jax.experimental.pallas import tpu as pltpu
from jax.sharding import Mesh
from jax.sharding import PartitionSpec as P

MEMBER = ("member_0", "member_1")
DP = ("dp_0", "dp_1", "dp_2")
AXES = MEMBER + DP
LANES = 128
F32 = jnp.float32
BF16 = jnp.bfloat16
NT = (((1,), (1,)), ((), ()))


def norm_rows(values, gain_row):
    values = values.astype(F32)
    center = values - jnp.mean(values, axis=-1, keepdims=True)
    spread = jnp.mean(center * center, axis=-1, keepdims=True)
    return center * lax.rsqrt(spread + 1e-06) * gain_row


def gamma_parts(x):
    small = x < 8.0
    base = jnp.where(small, x, 1.0)
    product = base
    harmonic = 1.0 / base
    for step in range(1, 8):
        product = product * (base + step)
        harmonic = harmonic + 1.0 / (base + step)
    big = jnp.where(small, x + 8.0, x)
    log_big = jnp.log(big)
    inv = 1.0 / big
    inv2 = inv * inv
    lgamma = (big - 0.5) * log_big - big + 0.9189385332046727
    lgamma = lgamma + inv * (1.0 / 12 - inv2 * (1.0 / 360 - inv2 * (1.0 / 1260)))
    digamma = log_big - 0.5 * inv - inv2 * (1.0 / 12 - inv2 * (1.0 / 120 - inv2 * (1.0 / 252)))
    lgamma = lgamma - jnp.where(small, jnp.log(product), 0.0)
    digamma = digamma - jnp.where(small, harmonic, 0.0)
    return lgamma, digamma


def start_copy(src, dst, send_sem, recv_sem, device):
    pltpu.make_async_remote_copy(
        src_ref=src,
        dst_ref=dst,
        send_sem=send_sem,
        recv_sem=recv_sem,
        device_id=device,
        device_id_type=pl.DeviceIdType.MESH,
    ).start()


def wait_bytes(ref, sem):
    pltpu.make_async_copy(ref, ref, sem).wait()


def step_kernel(
    sizes,
    tf_h, tg_h, w_h, tb_h, sf_h, sg_h, sh_h, sb_h,
    hg_o, bias_o, loss_o,
    tfv, tgv, wv, tbv, sfv, sgv, sbv, shv,
    xn, wt, tbt, lg, send, rb, tz, tb_s, tp,
    bm, bs, st, vs, vr,
    sn, sws, swr, swp, swq, swx, sbt, ad, asum, az, al_s,
    bc, bg_s, bgr, bh, bp, hs, hr, ht, hb, hp,
    ld, lz,
    in_sems, xn_sems, sn_sems, rb_sems, one, out,
):
    Z, H, Y, X, C = sizes
    z, h, y, x, c = (lax.axis_index(a) for a in AXES)
    dpn = Y * X * C
    me = (y * X + x) * C + c
    D = xn.shape[2]
    rows_t = xn.shape[1]
    L = wt.shape[0]
    cb = L // Z
    half_blocks = dpn // H
    ih = half_blocks * rows_t
    qb = half_blocks // 2
    iq = ih // 2
    rows_s = ih // Z
    q = rows_s // rows_t
    images = ih * H
    lane_half = LANES // H

    def at(nz=None, nh=None, ny=None, nx=None, nc=None):
        new = (nz, nh, ny, nx, nc)
        return tuple(old if n is None else n for old, n in zip((z, h, y, x, c), new))

    def spot(py, px, pc):
        d = (py * X + px) * C + pc
        m = d // q
        return (m % H) * half_blocks + (m // H) * q + d % q

    def ring(k):
        return lax.rem(z + k, Z)

    z_order = sorted(range(1, Z), key=lambda k: -min(k, Z - k))
    plane = [
        (lax.rem(y + i, Y), lax.rem(x + j, X), lax.rem(c + k, C))
        for i in reversed(range(Y))
        for j in range(X)
        for k in range(C)
        if i or j or k
    ]
    column = [y]
    if Y > 1:
        column.append(y + 1 - 2 * (y % 2))
    for k in range(2, Y):
        column.append((column[k - 2] + 2) % Y)
    groups = [range(0, Y // 2), range(Y // 2, Y)]
    first, second = groups
    near = [k for k in first if k]
    row_out = [lax.rem(x + j, X) for j in (2, 1, 3) if j < X]
    row_in = [lax.rem(x + j, X) for j in (1, 3, 2) if j < X]
    other = [lax.rem(c + e, C) for e in range(1, C)]

    loads = [
        pltpu.make_async_copy(src, dst, in_sems.at[i])
        for i, (src, dst) in enumerate(
            [
                (tf_h.at[0], tfv),
                (tg_h, tgv),
                (sf_h, sfv),
                (sg_h, sgv),
                (sh_h, shv),
                (tb_h, tbv),
                (sb_h, sbv),
                (w_h.at[0], wv),
            ]
        )
    ]
    for load in loads:
        load.start()
    barrier = pltpu.get_barrier_semaphore()
    peers = [at(ny=column[k]) for k in range(1, Y)] + [at(nx=px) for px in row_out]
    peers += [at(ny=column[k], nx=px) for k in near for px in row_out]
    peers += [at(nc=e) for e in other] + [at(nz=ring(k)) for k in range(1, Z)] + [at(nh=1 - h)]
    for peer in peers:
        pl.semaphore_signal(barrier, 1, device_id=peer, device_id_type=pl.DeviceIdType.MESH)

    own = spot(y, x, c)
    loads[0].wait()
    loads[1].wait()
    xn[own] = norm_rows(tfv[...], tgv[...]).astype(BF16)
    loads[2].wait()
    loads[3].wait()
    normed_s = norm_rows(sfv[...], sgv[...].reshape(1, D)).astype(BF16)
    sn[pl.ds(z * C, C)] = normed_s.reshape(C, rows_s // C, D)
    loads[4].wait()
    head = shv[...].astype(F32)
    blank = jnp.zeros_like(head)
    head = jnp.concatenate(
        [jnp.where(h == i, head, blank) for i in range(H)], axis=0
    ).T
    sws[...] = head.astype(BF16).reshape(Z, cb, LANES)
    pl.semaphore_wait(barrier, len(peers))

    def forward(block, device):
        start_copy(xn.at[block], xn.at[block], out.at[0], xn_sems.at[block], device)

    def arrived(block):
        wait_bytes(xn.at[block], xn_sems.at[block])

    def to_core(block):
        for e in other:
            forward(block, at(nc=e))

    for k in list(second) + near:
        forward(own, at(ny=column[k]))
    for k in [0] + near:
        for px in row_out:
            forward(own, at(ny=column[k], nx=px))
    to_core(own)
    for k in z_order:
        start_copy(sws.at[ring(k)], swr.at[z], out.at[3], one.at[1], at(nz=ring(k)))
    mine = z * C + c
    for k in z_order:
        start_copy(sn.at[mine], sn.at[mine], out.at[2], sn_sems.at[mine], at(nz=ring(k)))
    swr[z] = sws[z]

    loads[5].wait()
    loads[6].wait()
    tbt[...] = jnp.broadcast_to(tbv[...], (LANES, L)).T
    sbt[...] = jnp.broadcast_to(sbv[...].reshape(1, L), (LANES, L)).T
    loads[7].wait()
    for k in range(D // LANES):
        part = slice(k * LANES, (k + 1) * LANES)
        wt[:, part] = wv[part, :].astype(F32).T.astype(BF16)

    def from_core(k):
        for e in other:
            for px in [x] + row_in:
                arrived(spot(column[k], px, e))

    def logits_of(group):
        b = column[groups[group][0]] // (Y // 2)
        held = jnp.concatenate(
            [xn[pl.ds(a * half_blocks + b * qb, qb)].reshape(iq, D) for a in range(H)], axis=0
        )
        lg[...] = lax.dot_general(wt[...], held, NT, preferred_element_type=F32)
        for k in z_order + [0]:
            to = ring(k)
            rows = pl.ds(pl.multiple_of(to * cb, 16), cb)
            part = lg[rows, :] + tbt[rows, 0:1]
            top = jnp.max(part, axis=0, keepdims=True)
            part = part - top
            send[b, to] = part.astype(BF16)
            bm[b, to] = top
            bs[b, to] = jnp.sum(jnp.exp(part), axis=0, keepdims=True)
            if k:
                start_copy(send.at[b, to], rb.at[b, z], out.at[4 + 14 * group], rb_sems.at[group], at(nz=to))

    def pair_head():
        wait_bytes(swr.at[pl.ds(0, Z - 1)], one.at[1])
        for j in range(Z // 2):
            turned = pltpu.roll(swr[j + Z // 2].astype(F32), lane_half, 1)
            swp[j] = (swr[j].astype(F32) + turned).astype(BF16)
        start_copy(swp, swq, out.at[1], one.at[0], at(nh=1 - h))

    for k in near:
        block = spot(column[k], x, c)
        arrived(block)
        to_core(block)
    for k in second:
        block = spot(column[k], x, c)
        arrived(block)
        for px in row_out:
            forward(block, at(nx=px))
        to_core(block)
    for k in first:
        for px in row_in:
            block = spot(column[k], px, c)
            arrived(block)
            to_core(block)
    pair_head()
    for k in first:
        from_core(k)
    logits_of(0)
    for k in range(1, Z):
        block = ring(k) * C + c
        wait_bytes(sn.at[block], sn_sems.at[block])
        for e in other:
            start_copy(sn.at[block], sn.at[block], out.at[2], sn_sems.at[block], at(nc=e))
    for k in second:
        for px in row_in:
            block = spot(column[k], px, c)
            arrived(block)
            to_core(block)
    for k in second:
        from_core(k)
    logits_of(1)
    tops = bm[...]
    top = jnp.max(tops, axis=1)
    st[me] = top + jnp.log(jnp.sum(bs[...] * jnp.exp(tops - top[:, None]), axis=1))
    for a, b, e in plane:
        start_copy(st.at[me], st.at[me], out.at[5], one.at[2], at(ny=a, nx=b, nc=e))

    for e in other:
        for k in range(1, Z):
            block = ring(k) * C + e
            wait_bytes(sn.at[block], sn_sems.at[block])
    wait_bytes(swq, one.at[0])
    lane = lax.broadcasted_iota(jnp.int32, (cb, LANES), 1)
    theirs = jnp.where(lane >= lane_half, 1, 0) != h
    for j in range(Z // 2):
        packed = swq[j].astype(F32)
        turned = pltpu.roll(packed, lane_half, 1)
        for i, value in ((j, packed), (j + Z // 2, turned)):
            swx[i] = jnp.where(theirs, value, swr[i].astype(F32)).astype(BF16)
    scores = jnp.zeros((cb, ih), F32)
    for k in range(Z):
        part = slice(k * LANES, (k + 1) * LANES)
        scores = scores + lax.dot_general(
            swx[k], sn[:, :, part].reshape(ih, LANES), NT, preferred_element_type=F32
        )
    my_rows = pl.ds(pl.multiple_of(z * cb, 16), cb)
    alphas = jnp.exp(scores + sbt[my_rows, 0:1])
    al_s[...] = alphas
    ad[me] = jnp.sum(alphas, axis=0, keepdims=True)
    for a, b, e in plane:
        start_copy(ad.at[me], ad.at[me], out.at[6], one.at[3], at(ny=a, nx=b, nc=e))

    wait_bytes(st.at[pl.ds(0, dpn - 1)], one.at[2])
    tops = st[...]
    top = jnp.max(tops, axis=0)
    log_norm = top + jnp.log(jnp.sum(jnp.exp(tops - top[None]), axis=0))
    mine = z * H + h
    for b in range(2):
        shift = bm[b] - log_norm[b][None]
        for a in range(H):
            vs[:, a, b] = shift[:, :, a * iq : (a + 1) * iq]
    for k in z_order + [0]:
        start_copy(vs.at[ring(k), 1 - h], vr.at[mine], out.at[7], one.at[4], at(nz=ring(k), nh=1 - h))
    for k in z_order:
        start_copy(vs.at[ring(k), h], vr.at[mine], out.at[7], one.at[4], at(nz=ring(k)))
    vr[mine] = vs[z, h]

    wait_bytes(ad.at[pl.ds(0, dpn - 1)], one.at[3])
    asum[...] = jnp.sum(ad[...], axis=0)
    for k in z_order:
        start_copy(asum, az.at[z], out.at[8], one.at[5], at(nz=ring(k)))
    az[z] = asum[...]
    lgamma, digamma = gamma_parts(al_s[...])

    for group in range(2):
        b = column[groups[group][0]] // (Y // 2)
        wait_bytes(rb.at[b, pl.ds(0, Z - 1)], rb_sems.at[group])
        rb[b, z] = send[b, z]
        total = jnp.sum(rb[b].astype(F32), axis=0)
        for a in range(H):
            tz[a, b] = total[:, a * iq : (a + 1) * iq]
        tb_s[b] = tz[1 - h, b].astype(BF16)
        start_copy(tb_s.at[b], tp.at[b], out.at[9], one.at[6], at(nh=1 - h))
    wait_bytes(az.at[pl.ds(0, Z - 1)], one.at[5])
    lgamma_sum, digamma_sum = gamma_parts(jnp.sum(az[...], axis=0))
    wait_bytes(tp, one.at[6])
    wait_bytes(vr.at[pl.ds(0, Z * H - 1)], one.at[4])
    shift = jnp.sum(vr[...], axis=0)
    target = jnp.concatenate(
        [tz[h, b] + tp[b].astype(F32) + shift[b] for b in range(2)], axis=1
    ) / (Z * H)

    alphas = al_s[...]
    signal = alphas * (digamma - digamma_sum - target)
    terms = jnp.sum(lgamma - (alphas - 1.0) * target, axis=0, keepdims=True)
    terms = terms - lgamma_sum / (Z * dpn)
    deep = z * C + c
    ld[deep] = jnp.broadcast_to(jnp.sum(terms, axis=1, keepdims=True), (1, LANES))
    for k in z_order + [0]:
        for e in other + ([c] if k else []):
            start_copy(ld.at[deep], ld.at[deep], out.at[11], one.at[8], at(nz=ring(k), nc=e))

    high = signal.astype(BF16)
    rest = signal - high.astype(F32)
    mid = rest.astype(BF16)
    low = (rest - mid.astype(F32)).astype(BF16)
    parts = lax.dot_general(
        jnp.concatenate([high, mid, low], axis=0),
        sn[...].reshape(ih, D),
        (((1,), (0,)), ((), ())),
        preferred_element_type=F32,
    )
    grad = parts[:cb] + parts[cb : 2 * cb] + parts[2 * cb :]
    for k in range(Z):
        hs[k] = grad[:, k * LANES : (k + 1) * LANES].astype(BF16)
    for k in z_order:
        start_copy(hs.at[ring(k)], hr.at[z], out.at[12], one.at[9], at(nz=ring(k)))
    hr[z] = hs[z]
    bc[...] = jnp.zeros_like(bc)
    bc[my_rows, :] = jnp.broadcast_to(jnp.sum(signal, axis=1, keepdims=True), (cb, LANES))
    bg_s[...] = bc[...].T[0:1]
    for k in z_order:
        start_copy(bg_s, bgr.at[z], out.at[13], one.at[10], at(nz=ring(k)))
    bgr[z] = bg_s[...]

    wait_bytes(ld.at[pl.ds(0, Z * C - 1)], one.at[8])
    wide = (h * Y + y) * X + x
    lz[wide] = jnp.sum(ld[...], axis=0)
    for ph in (1 - h, h):
        for k in reversed(range(Y)):
            for px in row_out + ([x] if k or ph is not h else []):
                start_copy(lz.at[wide], lz.at[wide], out.at[14], one.at[11], at(nh=ph, ny=column[k], nx=px))

    wait_bytes(hr.at[pl.ds(0, Z - 1)], one.at[9])
    rows = hr[...].astype(F32).reshape(L, LANES).T
    ht[...] = rows.reshape(H, lane_half, L)
    hb[...] = ht[1 - h].astype(BF16)
    start_copy(hb, hp, out.at[15], one.at[12], at(nh=1 - h))
    wait_bytes(bgr.at[pl.ds(0, Z - 1)], one.at[10])
    bh[...] = jnp.sum(bgr[...], axis=0)
    start_copy(bh, bp, out.at[16], one.at[13], at(nh=1 - h))
    wait_bytes(hp, one.at[12])
    hg_o[...] = ht[h] + hp[...].astype(F32)
    wait_bytes(bp, one.at[13])
    bias_o[...] = ((bh[...] + bp[...]) / images).reshape(L)
    wait_bytes(lz.at[pl.ds(0, H * Y * X - 1)], one.at[11])
    loss_o[...] = jnp.sum(lz[...], axis=0) / (images * (L * dpn))

    sent = {
        0: xn.at[pl.ds(0, dpn - 1)],
        1: swp,
        2: sn.at[pl.ds(0, (Z - 1) * C)],
        3: sws.at[pl.ds(0, Z - 1)],
        4: send.at[0, pl.ds(0, Z - 1)],
        5: st.at[pl.ds(0, dpn - 1)],
        6: ad.at[pl.ds(0, dpn - 1)],
        7: vr.at[pl.ds(0, Z * H - 1)],
        8: az.at[pl.ds(0, Z - 1)],
        9: tb_s,
        11: ld.at[pl.ds(0, Z * C - 1)],
        12: hs.at[pl.ds(0, Z - 1)],
        13: bgr.at[pl.ds(0, Z - 1)],
        14: lz.at[pl.ds(0, H * Y * X - 1)],
        15: hb,
        16: bh,
        18: send.at[1, pl.ds(0, Z - 1)],
    }
    for i, ref in sent.items():
        wait_bytes(ref, out.at[i])


def on_device(sizes, tf, tg, w, tb, sf, sg, sh, sb):
    Z, H, Y, X, C = sizes
    dpn = Y * X * C
    rows_t, D = tf.shape[1:]
    L = w.shape[2]
    cb = L // Z
    ih = rows_t * dpn // H
    iq = ih // 2
    rows_s = sf.shape[0]
    images = ih * H
    assert D == Z * LANES and rows_s * Z == ih and sh.shape[0] * H == LANES

    def v(shape, dtype=F32):
        return pltpu.VMEM(shape, dtype)

    scratch = [
        v((rows_t, D), BF16), v((1, D)), v((D, L), BF16), v((1, L)),
        v((rows_s, D), BF16), v((D,)), v((L,)), v((LANES // H, L), BF16),
        v((dpn, rows_t, D), BF16), v((L, D), BF16), v((L, LANES)), v((L, ih)),
        v((2, Z, cb, ih), BF16), v((2, Z, cb, ih), BF16), v((H, 2, cb, iq)), v((2, cb, iq), BF16), v((2, cb, iq), BF16),
        v((2, Z, 1, ih)), v((2, Z, 1, ih)), v((dpn, 2, 1, ih)), v((Z, H, 2, 1, iq)), v((Z * H, 2, 1, iq)),
        v((Z * C, rows_s // C, D), BF16), v((Z, cb, LANES), BF16), v((Z, cb, LANES), BF16),
        v((Z // 2, cb, LANES), BF16), v((Z // 2, cb, LANES), BF16), v((Z, cb, LANES), BF16),
        v((L, LANES)), v((dpn, 1, ih)), v((1, ih)), v((Z, 1, ih)), v((cb, ih)),
        v((L, LANES)), v((1, L)), v((Z, 1, L)), v((1, L)), v((1, L)),
        v((Z, cb, LANES), BF16), v((Z, cb, LANES), BF16), v((H, LANES // H, L)),
        v((LANES // H, L), BF16), v((LANES // H, L), BF16),
        v((Z * C, 1, LANES)), v((H * Y * X, 1, LANES)),
        pltpu.SemaphoreType.DMA((8,)), pltpu.SemaphoreType.DMA((dpn,)), pltpu.SemaphoreType.DMA((Z * C,)),
        pltpu.SemaphoreType.DMA((2,)), pltpu.SemaphoreType.DMA((15,)), pltpu.SemaphoreType.DMA((19,)),
    ]
    vmem = pl.BlockSpec(memory_space=pltpu.VMEM)
    head_grad, bias_grad, loss = pl.pallas_call(
        functools.partial(step_kernel, sizes),
        out_shape=(
            jax.ShapeDtypeStruct((LANES // H, L), F32),
            jax.ShapeDtypeStruct((L,), F32),
            jax.ShapeDtypeStruct((1, LANES), F32),
        ),
        in_specs=[pl.BlockSpec(memory_space=pl.ANY)] * 8,
        out_specs=(vmem, vmem, vmem),
        scratch_shapes=scratch,
        compiler_params=pltpu.CompilerParams(
            collective_id=0, has_side_effects=True, vmem_limit_bytes=67043328
        ),
    )(tf, tg, w, tb, sf, sg, sh, sb)
    return loss[0, 0], head_grad / images, bias_grad


def solution(mesh, sizes=(8, 2, 4, 4, 2)):
    torus = Mesh(mesh.devices.reshape(sizes), AXES)
    placed = (
        P(MEMBER, DP, None),
        P(MEMBER, None),
        P(MEMBER, None, DP),
        P(MEMBER, DP),
        P(MEMBER, None),
        P(),
        P(MEMBER, DP),
        P(DP),
    )
    return jax.shard_map(
        functools.partial(on_device, sizes),
        mesh=torus,
        in_specs=placed,
        out_specs=(P(), P(MEMBER, DP), P(DP)),
        check_vma=False,
    )
```

```python
import functools

import jax
import jax.numpy as jnp
from jax import lax
from jax.experimental import pallas as pl
from jax.experimental.pallas import tpu as pltpu
from jax.sharding import Mesh
from jax.sharding import PartitionSpec as P

MEMBER = ("member_0", "member_1")
DP = ("dp_0", "dp_1", "dp_2")
AXES = MEMBER + DP
LANES = 128
F32 = jnp.float32
BF16 = jnp.bfloat16
NT = (((1,), (1,)), ((), ()))


def norm_rows(values, gain_row):
    values = values.astype(F32)
    center = values - jnp.mean(values, axis=-1, keepdims=True)
    spread = jnp.mean(center * center, axis=-1, keepdims=True)
    return center * lax.rsqrt(spread + 1e-06) * gain_row


def gamma_parts(x):
    small = x < 8.0
    base = jnp.where(small, x, 1.0)
    product = base
    harmonic = 1.0 / base
    for step in range(1, 8):
        product = product * (base + step)
        harmonic = harmonic + 1.0 / (base + step)
    big = jnp.where(small, x + 8.0, x)
    log_big = jnp.log(big)
    inv = 1.0 / big
    inv2 = inv * inv
    lgamma = (big - 0.5) * log_big - big + 0.9189385332046727
    lgamma = lgamma + inv * (1.0 / 12 - inv2 * (1.0 / 360 - inv2 * (1.0 / 1260)))
    digamma = log_big - 0.5 * inv - inv2 * (1.0 / 12 - inv2 * (1.0 / 120 - inv2 * (1.0 / 252)))
    lgamma = lgamma - jnp.where(small, jnp.log(product), 0.0)
    digamma = digamma - jnp.where(small, harmonic, 0.0)
    return lgamma, digamma


def start_copy(src, dst, send_sem, recv_sem, device):
    pltpu.make_async_remote_copy(
        src_ref=src,
        dst_ref=dst,
        send_sem=send_sem,
        recv_sem=recv_sem,
        device_id=device,
        device_id_type=pl.DeviceIdType.MESH,
    ).start()


def wait_bytes(ref, sem):
    pltpu.make_async_copy(ref, ref, sem).wait()


def step_kernel(
    sizes,
    tf_h, tg_h, w_h, tb_h, sf_h, sg_h, sh_h, sb_h,
    hg_o, bias_o, loss_o,
    tfv, tgv, wv, tbv, sfv, sgv, sbv, shv,
    xn, wt, tbt, lg, send, rb, tz, tb_s, tp,
    bm, bs, st, vs, vr,
    sn, sws, swr, swp, swq, swx, sbt, ad, asum, az, al_s,
    bc, bg_s, bgr, bh, bp, hs, hr, ht, hb, hp,
    ld, lz,
    in_sems, xn_sems, sn_sems, rb_sems, one, out,
):
    Z, H, Y, X, C = sizes
    z, h, y, x, c = (lax.axis_index(a) for a in AXES)
    dpn = Y * X * C
    me = (y * X + x) * C + c
    D = xn.shape[2]
    rows_t = xn.shape[1]
    L = wt.shape[0]
    cb = L // Z
    half_blocks = dpn // H
    ih = half_blocks * rows_t
    qb = half_blocks // 2
    iq = ih // 2
    rows_s = ih // Z
    q = rows_s // rows_t
    images = ih * H
    lane_half = LANES // H

    def at(nz=None, nh=None, ny=None, nx=None, nc=None):
        new = (nz, nh, ny, nx, nc)
        return tuple(old if n is None else n for old, n in zip((z, h, y, x, c), new))

    def spot(py, px, pc):
        d = (py * X + px) * C + pc
        m = d // q
        return (m % H) * half_blocks + (m // H) * q + d % q

    def ring(k):
        return lax.rem(z + k, Z)

    z_order = sorted(range(1, Z), key=lambda k: -min(k, Z - k))
    plane = [
        (lax.rem(y + i, Y), lax.rem(x + j, X), lax.rem(c + k, C))
        for i in reversed(range(Y))
        for j in range(X)
        for k in range(C)
        if i or j or k
    ]
    column = [y]
    if Y > 1:
        column.append(y + 1 - 2 * (y % 2))
    for k in range(2, Y):
        column.append((column[k - 2] + 2) % Y)
    groups = [range(0, Y // 2), range(Y // 2, Y)]
    first, second = groups
    near = [k for k in first if k]
    row_out = [lax.rem(x + j, X) for j in (2, 1, 3) if j < X]
    row_in = [lax.rem(x + j, X) for j in (1, 3, 2) if j < X]
    other = [lax.rem(c + e, C) for e in range(1, C)]

    loads = [
        pltpu.make_async_copy(src, dst, in_sems.at[i])
        for i, (src, dst) in enumerate(
            [
                (tf_h.at[0], tfv),
                (tg_h, tgv),
                (sf_h, sfv),
                (sg_h, sgv),
                (sh_h, shv),
                (tb_h, tbv),
                (sb_h, sbv),
                (w_h.at[0], wv),
            ]
        )
    ]
    for load in loads:
        load.start()
    barrier = pltpu.get_barrier_semaphore()
    peers = [at(ny=column[k]) for k in range(1, Y)] + [at(nx=px) for px in row_out]
    peers += [at(ny=column[k], nx=px) for k in near for px in row_out]
    peers += [at(nc=e) for e in other] + [at(nz=ring(k)) for k in range(1, Z)] + [at(nh=1 - h)]
    for peer in peers:
        pl.semaphore_signal(barrier, 1, device_id=peer, device_id_type=pl.DeviceIdType.MESH)

    own = spot(y, x, c)
    loads[0].wait()
    loads[1].wait()
    xn[own] = norm_rows(tfv[...], tgv[...]).astype(BF16)
    loads[2].wait()
    loads[3].wait()
    normed_s = norm_rows(sfv[...], sgv[...].reshape(1, D)).astype(BF16)
    sn[pl.ds(z * C, C)] = normed_s.reshape(C, rows_s // C, D)
    loads[4].wait()
    head = shv[...].astype(F32)
    blank = jnp.zeros_like(head)
    head = jnp.concatenate(
        [jnp.where(h == i, head, blank) for i in range(H)], axis=0
    ).T
    sws[...] = head.astype(BF16).reshape(Z, cb, LANES)
    pl.semaphore_wait(barrier, len(peers))

    def forward(block, device):
        start_copy(xn.at[block], xn.at[block], out.at[0], xn_sems.at[block], device)

    def arrived(block):
        wait_bytes(xn.at[block], xn_sems.at[block])

    def to_core(block):
        for e in other:
            forward(block, at(nc=e))

    for k in list(second) + near:
        forward(own, at(ny=column[k]))
    for k in [0] + near:
        for px in row_out:
            forward(own, at(ny=column[k], nx=px))
    to_core(own)
    for k in z_order:
        start_copy(sws.at[ring(k)], swr.at[z], out.at[3], one.at[1], at(nz=ring(k)))
    mine = z * C + c
    for k in z_order:
        start_copy(sn.at[mine], sn.at[mine], out.at[2], sn_sems.at[mine], at(nz=ring(k)))
    swr[z] = sws[z]

    loads[5].wait()
    loads[6].wait()
    tbt[...] = jnp.broadcast_to(tbv[...], (LANES, L)).T
    sbt[...] = jnp.broadcast_to(sbv[...].reshape(1, L), (LANES, L)).T
    loads[7].wait()
    for k in range(D // LANES):
        part = slice(k * LANES, (k + 1) * LANES)
        wt[:, part] = wv[part, :].astype(F32).T.astype(BF16)

    def from_core(k):
        for e in other:
            for px in [x] + row_in:
                arrived(spot(column[k], px, e))

    def logits_of(group):
        b = column[groups[group][0]] // (Y // 2)
        held = jnp.concatenate(
            [xn[pl.ds(a * half_blocks + b * qb, qb)].reshape(iq, D) for a in range(H)], axis=0
        )
        for part in (slice(0, L // 2), slice(L // 2, L)):
            lg[part, :] = lax.dot_general(wt[part, :], held, NT, preferred_element_type=F32)
        for to in range(Z):
            rows = slice(to * cb, (to + 1) * cb)
            part = lg[rows, :] + tbt[rows, 0:1]
            top = jnp.max(part, axis=0, keepdims=True)
            part = part - top
            send[b, to] = part.astype(BF16)
            bm[b, to] = top
            bs[b, to] = jnp.sum(jnp.exp(part), axis=0, keepdims=True)
        for k in z_order:
            to = ring(k)
            start_copy(
                send.at[b, to], rb.at[b, z], out.at[4 + 14 * group], rb_sems.at[group], at(nz=to)
            )

    def pair_head():
        wait_bytes(swr.at[pl.ds(0, Z - 1)], one.at[1])
        for j in range(Z // 2):
            turned = pltpu.roll(swr[j + Z // 2].astype(F32), lane_half, 1)
            swp[j] = (swr[j].astype(F32) + turned).astype(BF16)
        start_copy(swp, swq, out.at[1], one.at[0], at(nh=1 - h))

    for k in list(second) + near:
        block = spot(column[k], x, c)
        arrived(block)
        if k in second:
            for px in row_out:
                forward(block, at(nx=px))
        to_core(block)
    for k in first:
        for px in row_in:
            block = spot(column[k], px, c)
            arrived(block)
            to_core(block)
    pair_head()
    for k in first:
        from_core(k)
    logits_of(0)
    for k in second:
        for px in row_in:
            block = spot(column[k], px, c)
            arrived(block)
            to_core(block)
    for k in range(1, Z):
        block = ring(k) * C + c
        wait_bytes(sn.at[block], sn_sems.at[block])
        for e in other:
            start_copy(sn.at[block], sn.at[block], out.at[2], sn_sems.at[block], at(nc=e))
    for k in second:
        from_core(k)
    logits_of(1)
    tops = bm[...]
    top = jnp.max(tops, axis=1)
    st[me] = top + jnp.log(jnp.sum(bs[...] * jnp.exp(tops - top[:, None]), axis=1))
    for a, b, e in plane:
        start_copy(st.at[me], st.at[me], out.at[5], one.at[2], at(ny=a, nx=b, nc=e))

    for e in other:
        for k in range(1, Z):
            block = ring(k) * C + e
            wait_bytes(sn.at[block], sn_sems.at[block])
    wait_bytes(swq, one.at[0])
    lane = lax.broadcasted_iota(jnp.int32, (cb, LANES), 1)
    theirs = jnp.where(lane >= lane_half, 1, 0) != h
    for j in range(Z // 2):
        packed = swq[j].astype(F32)
        turned = pltpu.roll(packed, lane_half, 1)
        for i, value in ((j, packed), (j + Z // 2, turned)):
            swx[i] = jnp.where(theirs, value, swr[i].astype(F32)).astype(BF16)
    scores = jnp.zeros((cb, ih), F32)
    for k in range(Z):
        part = slice(k * LANES, (k + 1) * LANES)
        scores = scores + lax.dot_general(
            swx[k], sn[:, :, part].reshape(ih, LANES), NT, preferred_element_type=F32
        )
    my_rows = pl.ds(pl.multiple_of(z * cb, 16), cb)
    alphas = jnp.exp(scores + sbt[my_rows, 0:1])
    al_s[...] = alphas
    ad[me] = jnp.sum(alphas, axis=0, keepdims=True)
    for a, b, e in plane:
        start_copy(ad.at[me], ad.at[me], out.at[6], one.at[3], at(ny=a, nx=b, nc=e))

    wait_bytes(st.at[pl.ds(0, dpn - 1)], one.at[2])
    tops = st[...]
    top = jnp.max(tops, axis=0)
    log_norm = top + jnp.log(jnp.sum(jnp.exp(tops - top[None]), axis=0))
    mine = z * H + h
    for b in range(2):
        shift = bm[b] - log_norm[b][None]
        for a in range(H):
            vs[:, a, b] = shift[:, :, a * iq : (a + 1) * iq]
    for k in z_order + [0]:
        start_copy(vs.at[ring(k), 1 - h], vr.at[mine], out.at[7], one.at[4], at(nz=ring(k), nh=1 - h))
    for k in z_order:
        start_copy(vs.at[ring(k), h], vr.at[mine], out.at[7], one.at[4], at(nz=ring(k)))
    vr[mine] = vs[z, h]

    wait_bytes(ad.at[pl.ds(0, dpn - 1)], one.at[3])
    asum[...] = jnp.sum(ad[...], axis=0)
    for k in z_order:
        start_copy(asum, az.at[z], out.at[8], one.at[5], at(nz=ring(k)))
    az[z] = asum[...]
    lgamma, digamma = gamma_parts(al_s[...])

    for group in range(2):
        b = column[groups[group][0]] // (Y // 2)
        wait_bytes(rb.at[b, pl.ds(0, Z - 1)], rb_sems.at[group])
        rb[b, z] = send[b, z]
        total = jnp.sum(rb[b].astype(F32), axis=0)
        for a in range(H):
            tz[a, b] = total[:, a * iq : (a + 1) * iq]
        tb_s[b] = tz[1 - h, b].astype(BF16)
        start_copy(tb_s.at[b], tp.at[b], out.at[9], one.at[6], at(nh=1 - h))
    wait_bytes(az.at[pl.ds(0, Z - 1)], one.at[5])
    lgamma_sum, digamma_sum = gamma_parts(jnp.sum(az[...], axis=0))
    wait_bytes(tp, one.at[6])
    wait_bytes(vr.at[pl.ds(0, Z * H - 1)], one.at[4])
    shift = jnp.sum(vr[...], axis=0)
    target = jnp.concatenate(
        [tz[h, b] + tp[b].astype(F32) + shift[b] for b in range(2)], axis=1
    ) / (Z * H)

    alphas = al_s[...]
    signal = alphas * (digamma - digamma_sum - target)
    terms = jnp.sum(lgamma - (alphas - 1.0) * target, axis=0, keepdims=True)
    terms = terms - lgamma_sum / (Z * dpn)
    deep = z * C + c
    ld[deep] = jnp.broadcast_to(jnp.sum(terms, axis=1, keepdims=True), (1, LANES))
    for k in z_order + [0]:
        for e in other + ([c] if k else []):
            start_copy(ld.at[deep], ld.at[deep], out.at[11], one.at[8], at(nz=ring(k), nc=e))

    high = signal.astype(BF16)
    rest = signal - high.astype(F32)
    mid = rest.astype(BF16)
    low = (rest - mid.astype(F32)).astype(BF16)
    parts = lax.dot_general(
        jnp.concatenate([high, mid, low], axis=0),
        sn[...].reshape(ih, D),
        (((1,), (0,)), ((), ())),
        preferred_element_type=F32,
    )
    grad = parts[:cb] + parts[cb : 2 * cb] + parts[2 * cb :]
    for k in range(Z):
        hs[k] = grad[:, k * LANES : (k + 1) * LANES].astype(BF16)
    for k in z_order:
        start_copy(hs.at[ring(k)], hr.at[z], out.at[12], one.at[9], at(nz=ring(k)))
    hr[z] = hs[z]
    bc[...] = jnp.zeros_like(bc)
    bc[my_rows, :] = jnp.broadcast_to(jnp.sum(signal, axis=1, keepdims=True), (cb, LANES))
    bg_s[...] = bc[...].T[0:1]
    for k in z_order:
        start_copy(bg_s, bgr.at[z], out.at[13], one.at[10], at(nz=ring(k)))
    bgr[z] = bg_s[...]

    wait_bytes(ld.at[pl.ds(0, Z * C - 1)], one.at[8])
    wide = (h * Y + y) * X + x
    lz[wide] = jnp.sum(ld[...], axis=0)
    for ph in (1 - h, h):
        for k in reversed(range(Y)):
            for px in row_out + ([x] if k or ph is not h else []):
                start_copy(lz.at[wide], lz.at[wide], out.at[14], one.at[11], at(nh=ph, ny=column[k], nx=px))

    wait_bytes(hr.at[pl.ds(0, Z - 1)], one.at[9])
    rows = hr[...].astype(F32).reshape(L, LANES).T
    ht[...] = rows.reshape(H, lane_half, L)
    hb[...] = ht[1 - h].astype(BF16)
    start_copy(hb, hp, out.at[15], one.at[12], at(nh=1 - h))
    wait_bytes(bgr.at[pl.ds(0, Z - 1)], one.at[10])
    bh[...] = jnp.sum(bgr[...], axis=0)
    start_copy(bh, bp, out.at[16], one.at[13], at(nh=1 - h))
    wait_bytes(hp, one.at[12])
    hg_o[...] = ht[h] + hp[...].astype(F32)
    wait_bytes(bp, one.at[13])
    bias_o[...] = ((bh[...] + bp[...]) / images).reshape(L)
    wait_bytes(lz.at[pl.ds(0, H * Y * X - 1)], one.at[11])
    loss_o[...] = jnp.sum(lz[...], axis=0) / (images * (L * dpn))

    sent = {
        0: xn.at[pl.ds(0, dpn - 1)],
        1: swp,
        2: sn.at[pl.ds(0, (Z - 1) * C)],
        3: sws.at[pl.ds(0, Z - 1)],
        4: send.at[0, pl.ds(0, Z - 1)],
        5: st.at[pl.ds(0, dpn - 1)],
        6: ad.at[pl.ds(0, dpn - 1)],
        7: vr.at[pl.ds(0, Z * H - 1)],
        8: az.at[pl.ds(0, Z - 1)],
        9: tb_s,
        11: ld.at[pl.ds(0, Z * C - 1)],
        12: hs.at[pl.ds(0, Z - 1)],
        13: bgr.at[pl.ds(0, Z - 1)],
        14: lz.at[pl.ds(0, H * Y * X - 1)],
        15: hb,
        16: bh,
        18: send.at[1, pl.ds(0, Z - 1)],
    }
    for i, ref in sent.items():
        wait_bytes(ref, out.at[i])


def on_device(sizes, tf, tg, w, tb, sf, sg, sh, sb):
    Z, H, Y, X, C = sizes
    dpn = Y * X * C
    rows_t, D = tf.shape[1:]
    L = w.shape[2]
    cb = L // Z
    ih = rows_t * dpn // H
    iq = ih // 2
    rows_s = sf.shape[0]
    images = ih * H
    assert D == Z * LANES and rows_s * Z == ih and sh.shape[0] * H == LANES

    def v(shape, dtype=F32):
        return pltpu.VMEM(shape, dtype)

    scratch = [
        v((rows_t, D), BF16), v((1, D)), v((D, L), BF16), v((1, L)),
        v((rows_s, D), BF16), v((D,)), v((L,)), v((LANES // H, L), BF16),
        v((dpn, rows_t, D), BF16), v((L, D), BF16), v((L, LANES)), v((L, ih)),
        v((2, Z, cb, ih), BF16), v((2, Z, cb, ih), BF16), v((H, 2, cb, iq)), v((2, cb, iq), BF16), v((2, cb, iq), BF16),
        v((2, Z, 1, ih)), v((2, Z, 1, ih)), v((dpn, 2, 1, ih)), v((Z, H, 2, 1, iq)), v((Z * H, 2, 1, iq)),
        v((Z * C, rows_s // C, D), BF16), v((Z, cb, LANES), BF16), v((Z, cb, LANES), BF16),
        v((Z // 2, cb, LANES), BF16), v((Z // 2, cb, LANES), BF16), v((Z, cb, LANES), BF16),
        v((L, LANES)), v((dpn, 1, ih)), v((1, ih)), v((Z, 1, ih)), v((cb, ih)),
        v((L, LANES)), v((1, L)), v((Z, 1, L)), v((1, L)), v((1, L)),
        v((Z, cb, LANES), BF16), v((Z, cb, LANES), BF16), v((H, LANES // H, L)),
        v((LANES // H, L), BF16), v((LANES // H, L), BF16),
        v((Z * C, 1, LANES)), v((H * Y * X, 1, LANES)),
        pltpu.SemaphoreType.DMA((8,)), pltpu.SemaphoreType.DMA((dpn,)), pltpu.SemaphoreType.DMA((Z * C,)),
        pltpu.SemaphoreType.DMA((2,)), pltpu.SemaphoreType.DMA((15,)), pltpu.SemaphoreType.DMA((19,)),
    ]
    vmem = pl.BlockSpec(memory_space=pltpu.VMEM)
    head_grad, bias_grad, loss = pl.pallas_call(
        functools.partial(step_kernel, sizes),
        out_shape=(
            jax.ShapeDtypeStruct((LANES // H, L), F32),
            jax.ShapeDtypeStruct((L,), F32),
            jax.ShapeDtypeStruct((1, LANES), F32),
        ),
        in_specs=[pl.BlockSpec(memory_space=pl.ANY)] * 8,
        out_specs=(vmem, vmem, vmem),
        scratch_shapes=scratch,
        compiler_params=pltpu.CompilerParams(
            collective_id=0, has_side_effects=True, vmem_limit_bytes=48 * 2**20
        ),
    )(*(pltpu.with_memory_space_constraint(a, pltpu.HBM) for a in (tf, tg, w, tb, sf, sg, sh, sb)))
    return loss[0, 0], head_grad / images, bias_grad


def solution(mesh, sizes=(8, 2, 4, 4, 2)):
    torus = Mesh(mesh.devices.reshape(sizes), AXES)
    placed = (
        P(MEMBER, DP, None),
        P(MEMBER, None),
        P(MEMBER, None, DP),
        P(MEMBER, DP),
        P(MEMBER, None),
        P(),
        P(MEMBER, DP),
        P(DP),
    )
    return jax.shard_map(
        functools.partial(on_device, sizes),
        mesh=torus,
        in_specs=placed,
        out_specs=(P(), P(MEMBER, DP), P(DP)),
        check_vma=False,
    )
```

```python
import functools
import math

import jax
import jax.numpy as jnp
from jax import lax
from jax.experimental import pallas as pl
from jax.experimental.pallas import tpu as pltpu
from jax.sharding import Mesh
from jax.sharding import PartitionSpec as P

MEMBER = ("member_0", "member_1")
DP = ("dp_0", "dp_1", "dp_2")
AXES = MEMBER + DP
LANES = 128
F32 = jnp.float32
BF16 = jnp.bfloat16
NT = (((1,), (1,)), ((), ()))


def norm_rows(values, gain_row):
    values = values.astype(F32)
    center = values - jnp.mean(values, axis=-1, keepdims=True)
    spread = jnp.mean(center * center, axis=-1, keepdims=True)
    return center * lax.rsqrt(spread + 1e-06) * gain_row


def gamma_parts(x):
    small = x < 8.0
    base = jnp.where(small, x, 1.0)
    product = base
    harmonic = 1.0 / base
    for step in range(1, 8):
        product = product * (base + step)
        harmonic = harmonic + 1.0 / (base + step)
    big = jnp.where(small, x + 8.0, x)
    log_big = jnp.log(big)
    inv = 1.0 / big
    inv2 = inv * inv
    lgamma = (big - 0.5) * log_big - big + 0.9189385332046727
    lgamma = lgamma + inv * (1.0 / 12 - inv2 * (1.0 / 360 - inv2 * (1.0 / 1260)))
    digamma = log_big - 0.5 * inv - inv2 * (1.0 / 12 - inv2 * (1.0 / 120 - inv2 * (1.0 / 252)))
    lgamma = lgamma - jnp.where(small, jnp.log(product), 0.0)
    digamma = digamma - jnp.where(small, harmonic, 0.0)
    return lgamma, digamma


def wait_bytes(ref, sem):
    pltpu.make_async_copy(ref, ref, sem).wait()


def step_kernel(
    sizes,
    tf_h, tg_h, w_h, tb_h, sf_h, sg_h, sh_h, sb_h,
    hg_o, bias_o, loss_o,
    tfv, tgv, wv, tbv, sfv, sgv, sbv, shv,
    xn, wt, tbt, lg, send, rb, tz, tb_s, tp,
    bm, st, vs, vr,
    sn, sws, swr, swp, swq, swx, sbt, ad, asum, az, al_s,
    bc, bg_s, bgr, bh, bp, hs, hr, ht, hb, hp,
    ld, lz,
    tally, in_sems, xn_sems, core_sems, sn_sems, rb_sems, st_sems, one, out_sems,
):
    Z, H, Y, X, C = sizes
    z, h, y, x, c = (lax.axis_index(a) for a in AXES)
    dpn = Y * X * C
    me = (y * X + x) * C + c
    D = xn.shape[2]
    rows_t = xn.shape[1]
    L = wt.shape[0]
    cb = L // Z
    half_blocks = dpn // H
    ih = half_blocks * rows_t
    qb = half_blocks // 2
    iq = ih // 2
    rows_s = ih // Z
    q = rows_s // rows_t
    images = ih * H
    lane_half = LANES // H

    sent = []
    out = out_sems.at[0]

    def start_copy(src, dst, recv_sem, device):
        sent.append(math.prod(src.shape) * src.dtype.itemsize)
        pltpu.make_async_remote_copy(
            src_ref=src,
            dst_ref=dst,
            send_sem=out,
            recv_sem=recv_sem,
            device_id=device,
            device_id_type=pl.DeviceIdType.MESH,
        ).start()

    def wait_sum(sizes, sem):
        wait_bytes(tally.at[pl.ds(0, sum(sizes) // (2 * LANES))], sem)

    def at(nz=None, nh=None, ny=None, nx=None, nc=None):
        new = (nz, nh, ny, nx, nc)
        return tuple(old if n is None else n for old, n in zip((z, h, y, x, c), new))

    def spot(py, px, pc):
        d = (py * X + px) * C + pc
        m = d // q
        return (m % H) * half_blocks + (m // H) * q + d % q

    def ring(k):
        return lax.rem(z + k, Z)

    z_order = sorted(range(1, Z), key=lambda k: -min(k, Z - k))
    plane = [
        (lax.rem(y + i, Y), lax.rem(x + j, X), lax.rem(c + k, C))
        for i in reversed(range(Y))
        for j in range(X)
        for k in range(C)
        if i or j or k
    ]
    column = [y]
    if Y > 1:
        column.append(y + 1 - 2 * (y % 2))
    for k in range(2, Y):
        column.append((column[k - 2] + 2) % Y)
    groups = [range(0, Y // 2), range(Y // 2, Y)]
    first, second = groups
    near = [k for k in first if k]
    row_out = [lax.rem(x + j, X) for j in (2, 1, 3) if j < X]
    row_in = [lax.rem(x + j, X) for j in (1, 3, 2) if j < X]
    other = [lax.rem(c + e, C) for e in range(1, C)]

    loads = []
    for i, group in enumerate(
        [
            [(tf_h.at[0], tfv), (tg_h, tgv)],
            [(sf_h, sfv), (sg_h, sgv), (sh_h, shv)],
            [(tb_h, tbv), (sb_h, sbv), (w_h.at[0], wv)],
        ]
    ):
        for src, dst in group:
            pltpu.make_async_copy(src, dst, in_sems.at[i]).start()
        loads.append([math.prod(dst.shape) * dst.dtype.itemsize for _, dst in group])
    barrier = pltpu.get_barrier_semaphore()
    peers = [at(ny=column[k]) for k in range(1, Y)] + [at(nx=px) for px in row_out]
    peers += [at(ny=column[k], nx=px) for k in near for px in row_out]
    peers += [at(nc=e) for e in other] + [at(nz=ring(k)) for k in range(1, Z)] + [at(nh=1 - h)]
    for peer in peers:
        pl.semaphore_signal(barrier, 1, device_id=peer, device_id_type=pl.DeviceIdType.MESH)

    own = spot(y, x, c)
    wait_sum(loads[0], in_sems.at[0])
    xn[own] = norm_rows(tfv[...], tgv[...]).astype(BF16)
    pl.semaphore_wait(barrier, len(peers))

    def forward(k, px, device):
        block = spot(column[k], px, c)
        start_copy(xn.at[block], xn.at[block], xn_sems.at[column[k] * X + px], device)

    def arrived(k, px):
        wait_bytes(xn.at[spot(column[k], px, c)], xn_sems.at[column[k] * X + px])

    def to_core(k, px):
        block = spot(column[k], px, c)
        for e in other:
            start_copy(xn.at[block], xn.at[block], core_sems.at[int(k in second)], at(nc=e))

    for k in list(second) + near:
        forward(0, x, at(ny=column[k]))
    for k in [0] + near:
        for px in row_out:
            forward(0, x, at(ny=column[k], nx=px))
    to_core(0, x)
    wait_sum(loads[1], in_sems.at[1])
    head = shv[...].astype(F32)
    blank = jnp.zeros_like(head)
    head = jnp.concatenate([jnp.where(h == i, head, blank) for i in range(H)], axis=0).T
    sws[...] = head.astype(BF16).reshape(Z, cb, LANES)
    for k in z_order:
        start_copy(sws.at[ring(k)], swr.at[z], one.at[1], at(nz=ring(k)))
    swr[z] = sws[z]
    normed_s = norm_rows(sfv[...], sgv[...].reshape(1, D)).astype(BF16)
    sn[pl.ds(z * C, C)] = normed_s.reshape(C, rows_s // C, D)
    mine = z * C + c
    for k in z_order:
        start_copy(sn.at[mine], sn.at[mine], sn_sems.at[z], at(nz=ring(k)))

    wait_sum(loads[2], in_sems.at[2])
    tbt[...] = jnp.broadcast_to(tbv[...], (LANES, L)).T
    sbt[...] = jnp.broadcast_to(sbv[...].reshape(1, L), (LANES, L)).T
    for k in range(D // LANES):
        part = slice(k * LANES, (k + 1) * LANES)
        wt[:, part] = wv[part, :].astype(F32).T.astype(BF16)

    def from_core(group):
        if other:
            wait_bytes(xn.at[pl.ds(0, len(groups[group]) * X)], core_sems.at[group])

    def logits_of(group):
        b = column[groups[group][0]] // (Y // 2)
        held = jnp.concatenate(
            [xn[pl.ds(a * half_blocks + b * qb, qb)].reshape(iq, D) for a in range(H)], axis=0
        )
        for part in (slice(0, L // 2), slice(L // 2, L)):
            lg[part, :] = lax.dot_general(wt[part, :], held, NT, preferred_element_type=F32)
        tops, sums = [], []
        for to in range(Z):
            rows = slice(to * cb, (to + 1) * cb)
            part = lg[rows, :] + tbt[rows, 0:1]
            top = jnp.max(part, axis=0, keepdims=True)
            part = part - top
            for a in range(H):
                send[b, a, to] = part[:, a * iq : (a + 1) * iq].astype(BF16)
            bm[b, to] = top
            tops.append(top)
            sums.append(jnp.sum(jnp.exp(part), axis=0, keepdims=True))
        for i, a in enumerate((1 - h, h)):
            for k in z_order:
                to = ring(k)
                start_copy(send.at[b, a, to], rb.at[b, a, z], rb_sems.at[2 * group + i], at(nz=to))
        top = functools.reduce(jnp.maximum, tops)
        st[b, me] = top + jnp.log(sum(v * jnp.exp(t - top) for v, t in zip(sums, tops)))
        for ny, nx, nc in plane:
            start_copy(st.at[b, me], st.at[b, me], st_sems.at[group], at(ny=ny, nx=nx, nc=nc))

    def pair_head():
        wait_bytes(swr.at[pl.ds(0, Z - 1)], one.at[1])
        for j in range(Z // 2):
            turned = pltpu.roll(swr[j + Z // 2].astype(F32), lane_half, 1)
            swp[j] = (swr[j].astype(F32) + turned).astype(BF16)
        start_copy(swp, swq, one.at[0], at(nh=1 - h))

    for k in list(second) + near:
        arrived(k, x)
        if k in second:
            for px in row_out:
                forward(k, x, at(nx=px))
        to_core(k, x)
    for k in first:
        for px in row_in:
            arrived(k, px)
            to_core(k, px)
    pair_head()
    from_core(0)
    logits_of(0)
    for k in second:
        for px in row_in:
            arrived(k, px)
            to_core(k, px)
    for k in range(1, Z):
        block = ring(k) * C + c
        wait_bytes(sn.at[block], sn_sems.at[ring(k)])
        for e in other:
            start_copy(sn.at[block], sn.at[block], core_sems.at[2], at(nc=e))
    from_core(1)
    logits_of(1)

    if other:
        wait_bytes(sn.at[pl.ds(0, Z - 1)], core_sems.at[2])
    wait_bytes(swq, one.at[0])
    lane = lax.broadcasted_iota(jnp.int32, (cb, LANES), 1)
    theirs = jnp.where(lane >= lane_half, 1, 0) != h
    for j in range(Z // 2):
        packed = swq[j].astype(F32)
        turned = pltpu.roll(packed, lane_half, 1)
        for i, value in ((j, packed), (j + Z // 2, turned)):
            swx[i] = jnp.where(theirs, value, swr[i].astype(F32)).astype(BF16)
    scores = jnp.zeros((cb, ih), F32)
    for k in range(Z):
        part = slice(k * LANES, (k + 1) * LANES)
        scores = scores + lax.dot_general(
            swx[k], sn[:, :, part].reshape(ih, LANES), NT, preferred_element_type=F32
        )
    my_rows = pl.ds(pl.multiple_of(z * cb, 16), cb)
    alphas = jnp.exp(scores + sbt[my_rows, 0:1])
    al_s[...] = alphas
    ad[me] = jnp.sum(alphas, axis=0, keepdims=True)
    for a, b, e in plane:
        start_copy(ad.at[me], ad.at[me], one.at[2], at(ny=a, nx=b, nc=e))

    for group in range(2):
        b = column[groups[group][0]] // (Y // 2)
        wait_bytes(st.at[b, pl.ds(0, dpn - 1)], st_sems.at[group])
    tops = st[...]
    top = jnp.max(tops, axis=1)
    log_norm = top + jnp.log(jnp.sum(jnp.exp(tops - top[:, None]), axis=1))
    mine = z * H + h
    for b in range(2):
        shift = bm[b] - log_norm[b][None]
        for a in range(H):
            vs[:, a, b] = shift[:, :, a * iq : (a + 1) * iq]
    for k in z_order + [0]:
        start_copy(vs.at[ring(k), 1 - h], vr.at[mine], one.at[3], at(nz=ring(k), nh=1 - h))
    for k in z_order:
        start_copy(vs.at[ring(k), h], vr.at[mine], one.at[3], at(nz=ring(k)))
    vr[mine] = vs[z, h]

    halves = [column[group[0]] // (Y // 2) for group in groups]

    def summed(group, i):
        b, a = halves[group], (1 - h, h)[i]
        wait_bytes(rb.at[b, a, pl.ds(0, Z - 1)], rb_sems.at[2 * group + i])
        rb[b, a, z] = send[b, a, z]
        return b, jnp.sum(rb[b, a].astype(F32), axis=0)

    def to_partner(group):
        b, total = summed(group, 0)
        tb_s[b] = total.astype(BF16)
        start_copy(tb_s.at[b], tp.at[b], one.at[5], at(nh=1 - h))

    to_partner(0)
    wait_bytes(ad.at[pl.ds(0, dpn - 1)], one.at[2])
    asum[...] = jnp.sum(ad[...], axis=0)
    for k in z_order:
        start_copy(asum, az.at[z], one.at[4], at(nz=ring(k)))
    az[z] = asum[...]
    lgamma, digamma = gamma_parts(al_s[...])
    to_partner(1)
    for group in range(2):
        b, total = summed(group, 1)
        tz[b] = total
    wait_bytes(az.at[pl.ds(0, Z - 1)], one.at[4])
    lgamma_sum, digamma_sum = gamma_parts(jnp.sum(az[...], axis=0))
    wait_bytes(tp, one.at[5])
    wait_bytes(vr.at[pl.ds(0, Z * H - 1)], one.at[3])
    shift = jnp.sum(vr[...], axis=0)
    target = jnp.concatenate(
        [tz[b] + tp[b].astype(F32) + shift[b] for b in range(2)], axis=1
    ) / (Z * H)

    alphas = al_s[...]
    signal = alphas * (digamma - digamma_sum - target)
    terms = jnp.sum(lgamma - (alphas - 1.0) * target, axis=0, keepdims=True)
    terms = terms - lgamma_sum / (Z * dpn)
    deep = z * C + c
    ld[deep] = jnp.broadcast_to(jnp.sum(terms, axis=1, keepdims=True), (1, LANES))
    for k in z_order + [0]:
        for e in other + ([c] if k else []):
            start_copy(ld.at[deep], ld.at[deep], one.at[6], at(nz=ring(k), nc=e))

    high = signal.astype(BF16)
    rest = signal - high.astype(F32)
    mid = rest.astype(BF16)
    low = (rest - mid.astype(F32)).astype(BF16)
    parts = lax.dot_general(
        jnp.concatenate([high, mid, low], axis=0),
        sn[...].reshape(ih, D),
        (((1,), (0,)), ((), ())),
        preferred_element_type=F32,
    )
    grad = parts[:cb] + parts[cb : 2 * cb] + parts[2 * cb :]
    for k in range(Z):
        hs[k] = grad[:, k * LANES : (k + 1) * LANES].astype(BF16)
    for k in z_order:
        start_copy(hs.at[ring(k)], hr.at[z], one.at[7], at(nz=ring(k)))
    hr[z] = hs[z]
    bc[...] = jnp.zeros_like(bc)
    bc[my_rows, :] = jnp.broadcast_to(jnp.sum(signal, axis=1, keepdims=True), (cb, LANES))
    bg_s[...] = bc[...].T[0:1]
    for k in z_order:
        start_copy(bg_s, bgr.at[z], one.at[8], at(nz=ring(k)))
    bgr[z] = bg_s[...]

    wait_bytes(ld.at[pl.ds(0, Z * C - 1)], one.at[6])
    wide = (h * Y + y) * X + x
    lz[wide] = jnp.sum(ld[...], axis=0)
    for ph in (1 - h, h):
        for k in reversed(range(Y)):
            for px in row_out + ([x] if k or ph is not h else []):
                start_copy(lz.at[wide], lz.at[wide], one.at[9], at(nh=ph, ny=column[k], nx=px))

    wait_bytes(hr.at[pl.ds(0, Z - 1)], one.at[7])
    rows = hr[...].astype(F32).reshape(L, LANES).T
    ht[...] = rows.reshape(H, lane_half, L)
    hb[...] = ht[1 - h].astype(BF16)
    start_copy(hb, hp, one.at[10], at(nh=1 - h))
    wait_bytes(bgr.at[pl.ds(0, Z - 1)], one.at[8])
    bh[...] = jnp.sum(bgr[...], axis=0)
    start_copy(bh, bp, one.at[11], at(nh=1 - h))
    wait_bytes(hp, one.at[10])
    hg_o[...] = ht[h] + hp[...].astype(F32)
    wait_bytes(bp, one.at[11])
    bias_o[...] = ((bh[...] + bp[...]) / images).reshape(L)
    wait_bytes(lz.at[pl.ds(0, H * Y * X - 1)], one.at[9])
    loss_o[...] = jnp.sum(lz[...], axis=0) / (images * (L * dpn))

    wait_sum(sent, out)


def on_device(sizes, tf, tg, w, tb, sf, sg, sh, sb):
    Z, H, Y, X, C = sizes
    dpn = Y * X * C
    rows_t, D = tf.shape[1:]
    L = w.shape[2]
    cb = L // Z
    ih = rows_t * dpn // H
    iq = ih // 2
    rows_s = sf.shape[0]
    images = ih * H
    assert D == Z * LANES and rows_s * Z == ih and sh.shape[0] * H == LANES

    def v(shape, dtype=F32):
        return pltpu.VMEM(shape, dtype)

    scratch = [
        v((rows_t, D), BF16), v((1, D)), v((D, L), BF16), v((1, L)),
        v((rows_s, D), BF16), v((D,)), v((L,)), v((LANES // H, L), BF16),
        v((dpn, rows_t, D), BF16), v((L, D), BF16), v((L, LANES)), v((L, ih)),
        v((2, H, Z, cb, iq), BF16), v((2, H, Z, cb, iq), BF16), v((2, cb, iq)), v((2, cb, iq), BF16), v((2, cb, iq), BF16),
        v((2, Z, 1, ih)), v((2, dpn, 1, ih)), v((Z, H, 2, 1, iq)), v((Z * H, 2, 1, iq)),
        v((Z * C, rows_s // C, D), BF16), v((Z, cb, LANES), BF16), v((Z, cb, LANES), BF16),
        v((Z // 2, cb, LANES), BF16), v((Z // 2, cb, LANES), BF16), v((Z, cb, LANES), BF16),
        v((L, LANES)), v((dpn, 1, ih)), v((1, ih)), v((Z, 1, ih)), v((cb, ih)),
        v((L, LANES)), v((1, L)), v((Z, 1, L)), v((1, L)), v((1, L)),
        v((Z, cb, LANES), BF16), v((Z, cb, LANES), BF16), v((H, LANES // H, L)),
        v((LANES // H, L), BF16), v((LANES // H, L), BF16),
        v((Z * C, 1, LANES)), v((H * Y * X, 1, LANES)),
        v((2**15, LANES), BF16),
        pltpu.SemaphoreType.DMA((3,)), pltpu.SemaphoreType.DMA((Y * X,)), pltpu.SemaphoreType.DMA((3,)),
        pltpu.SemaphoreType.DMA((Z,)), pltpu.SemaphoreType.DMA((4,)), pltpu.SemaphoreType.DMA((2,)),
        pltpu.SemaphoreType.DMA((12,)), pltpu.SemaphoreType.DMA((1,)),
    ]
    vmem = pl.BlockSpec(memory_space=pltpu.VMEM)
    head_grad, bias_grad, loss = pl.pallas_call(
        functools.partial(step_kernel, sizes),
        out_shape=(
            jax.ShapeDtypeStruct((LANES // H, L), F32),
            jax.ShapeDtypeStruct((L,), F32),
            jax.ShapeDtypeStruct((1, LANES), F32),
        ),
        in_specs=[pl.BlockSpec(memory_space=pl.ANY)] * 8,
        out_specs=(vmem, vmem, vmem),
        scratch_shapes=scratch,
        compiler_params=pltpu.CompilerParams(
            collective_id=0, has_side_effects=True, vmem_limit_bytes=48 * 2**20
        ),
    )(*(pltpu.with_memory_space_constraint(a, pltpu.HBM) for a in (tf, tg, w, tb, sf, sg, sh, sb)))
    return loss[0, 0], head_grad / images, bias_grad


def solution(mesh, sizes=(8, 2, 4, 4, 2)):
    torus = Mesh(mesh.devices.reshape(sizes), AXES)
    placed = (
        P(MEMBER, DP, None),
        P(MEMBER, None),
        P(MEMBER, None, DP),
        P(MEMBER, DP),
        P(MEMBER, None),
        P(),
        P(MEMBER, DP),
        P(DP),
    )
    return jax.shard_map(
        functools.partial(on_device, sizes),
        mesh=torus,
        in_specs=placed,
        out_specs=(P(), P(MEMBER, DP), P(DP)),
        check_vma=False,
    )
```

```python
import functools
import math

import jax
import jax.numpy as jnp
from jax import lax
from jax.experimental import pallas as pl
from jax.experimental.pallas import tpu as pltpu
from jax.sharding import Mesh
from jax.sharding import PartitionSpec as P

MEMBER = ("member_0", "member_1")
DP = ("dp_0", "dp_1", "dp_2")
AXES = MEMBER + DP
LANES = 128
F32 = jnp.float32
BF16 = jnp.bfloat16
NT = (((1,), (1,)), ((), ()))


def norm_rows(values, gain_row):
    values = values.astype(F32)
    center = values - jnp.mean(values, axis=-1, keepdims=True)
    spread = jnp.mean(center * center, axis=-1, keepdims=True)
    return center * lax.rsqrt(spread + 1e-06) * gain_row


def gamma_parts(x):
    small = x < 8.0
    base = jnp.where(small, x, 1.0)
    product = base
    harmonic = 1.0 / base
    for step in range(1, 8):
        product = product * (base + step)
        harmonic = harmonic + 1.0 / (base + step)
    big = jnp.where(small, x + 8.0, x)
    log_big = jnp.log(big)
    inv = 1.0 / big
    inv2 = inv * inv
    lgamma = (big - 0.5) * log_big - big + 0.9189385332046727
    lgamma = lgamma + inv * (1.0 / 12 - inv2 * (1.0 / 360 - inv2 * (1.0 / 1260)))
    digamma = log_big - 0.5 * inv - inv2 * (1.0 / 12 - inv2 * (1.0 / 120 - inv2 * (1.0 / 252)))
    lgamma = lgamma - jnp.where(small, jnp.log(product), 0.0)
    digamma = digamma - jnp.where(small, harmonic, 0.0)
    return lgamma, digamma


def wait_bytes(ref, sem):
    pltpu.make_async_copy(ref, ref, sem).wait()


def step_kernel(
    sizes,
    tf_h, tg_h, w_h, tb_h, sf_h, sg_h, sh_h, sb_h,
    hg_o, bias_o, loss_o,
    tfv, tgv, wv, tbv, sfv, sgv, sbv, shv,
    xn, wt, tbt, lg, send, rb, tz, tb_s, tp,
    bm, br, st, vs, vr,
    sn, sws, swr, swp, swq, swx, sbt, ad, asum, az, al_s,
    bc, bg_s, bgr, bh, bp, hs, hr, ht, hb, hp,
    ld, lz,
    tally, in_sems, xn_sems, core_sems, sn_sems, rb_sems, st_sems, br_sems, one, out_sems,
):
    Z, H, Y, X, C = sizes
    z, h, y, x, c = (lax.axis_index(a) for a in AXES)
    dpn = Y * X * C
    me = (y * X + x) * C + c
    D = xn.shape[2]
    rows_t = xn.shape[1]
    L = wt.shape[0]
    cb = L // Z
    half_blocks = dpn // H
    ih = half_blocks * rows_t
    qb = half_blocks // 2
    iq = ih // 2
    rows_s = ih // Z
    q = rows_s // rows_t
    images = ih * H
    lane_half = LANES // H

    hub = C - 1
    sent = [[], [], []]

    def start_copy(src, dst, recv_sem, device, kind=0):
        sent[kind].append(math.prod(src.shape) * src.dtype.itemsize)
        pltpu.make_async_remote_copy(
            src_ref=src,
            dst_ref=dst,
            send_sem=out_sems.at[kind],
            recv_sem=recv_sem,
            device_id=device,
            device_id_type=pl.DeviceIdType.MESH,
        ).start()

    def to_own_hub(ref, recv_sem):
        if C > 1:

            @pl.when(c != hub)
            def _():
                start_copy(ref, ref, recv_sem, at(nc=hub), 2)

    def wait_from_hubs(ref, count, sem):
        @pl.when(c == hub)
        def _():
            wait_bytes(ref.at[pl.ds(0, count - 1)], sem)

        if C > 1:

            @pl.when(c != hub)
            def _():
                wait_bytes(ref.at[pl.ds(0, count)], sem)

    def wait_sum(sizes, sem):
        wait_bytes(tally.at[pl.ds(0, sum(sizes) // (2 * LANES))], sem)

    def at(nz=None, nh=None, ny=None, nx=None, nc=None):
        new = (nz, nh, ny, nx, nc)
        return tuple(old if n is None else n for old, n in zip((z, h, y, x, c), new))

    def spot(py, px, pc):
        d = (py * X + px) * C + pc
        m = d // q
        return (m % H) * half_blocks + (m // H) * q + d % q

    def ring(k):
        return lax.rem(z + k, Z)

    z_order = sorted(range(1, Z), key=lambda k: -min(k, Z - k))
    plane = [
        (lax.rem(y + i, Y), lax.rem(x + j, X)) for i in reversed(range(Y)) for j in range(X) if i or j
    ]
    column = [y]
    if Y > 1:
        column.append(y + 1 - 2 * (y % 2))
    for k in range(2, Y):
        column.append((column[k - 2] + 2) % Y)
    groups = [range(0, Y // 2), range(Y // 2, Y)]
    first, second = groups
    halves = [column[group[0]] // (Y // 2) for group in groups]
    near = [k for k in first if k]
    row_out = [lax.rem(x + j, X) for j in (2, 1, 3) if j < X]
    row_in = [lax.rem(x + j, X) for j in (1, 3, 2) if j < X]
    other = [lax.rem(c + e, C) for e in range(1, C)]
    twin = (other + [c])[0]

    loads = []
    for i, group in enumerate(
        [
            [(tf_h.at[0], tfv), (tg_h, tgv)],
            [(sf_h, sfv), (sg_h, sgv), (sh_h, shv)],
            [(tb_h, tbv), (sb_h, sbv), (w_h.at[0], wv)],
        ]
    ):
        for src, dst in group:
            pltpu.make_async_copy(src, dst, in_sems.at[i]).start()
        loads.append([math.prod(dst.shape) * dst.dtype.itemsize for _, dst in group])
    barrier = pltpu.get_barrier_semaphore()
    peers = [at(ny=column[k], nc=twin) for k in range(1, Y)]
    peers += [at(nx=px, nc=twin) for px in row_out]
    peers += [at(ny=column[k], nx=px, nc=twin) for k in near for px in row_out]
    peers += [at(nc=e) for e in other] + [at(nz=ring(k)) for k in range(1, Z)] + [at(nh=1 - h)]
    peers += [at(nz=ring(k), nc=e) for k in range(1, Z) for e in other]
    for peer in peers:
        pl.semaphore_signal(barrier, 1, device_id=peer, device_id_type=pl.DeviceIdType.MESH)

    own = spot(y, x, c)
    wait_sum(loads[0], in_sems.at[0])
    xn[own] = norm_rows(tfv[...], tgv[...]).astype(BF16)
    pl.semaphore_wait(barrier, len(peers))

    def origin(k, px):
        if k == 0 and px is x:
            return c
        return c if k in second and px is not x else twin

    def forward(k, px, device):
        block = spot(column[k], px, origin(k, px))
        start_copy(xn.at[block], xn.at[block], xn_sems.at[column[k] * X + px], device)

    def arrived(k, px):
        wait_bytes(xn.at[spot(column[k], px, origin(k, px))], xn_sems.at[column[k] * X + px])

    def to_core(k, px):
        block = spot(column[k], px, origin(k, px))
        for e in other:
            start_copy(xn.at[block], xn.at[block], core_sems.at[int(k in second)], at(nc=e))

    for k in list(second) + near:
        forward(0, x, at(ny=column[k], nc=twin))
    for k in [0] + near:
        for px in row_out:
            forward(0, x, at(ny=column[k], nx=px, nc=twin))
    to_core(0, x)
    wait_sum(loads[1], in_sems.at[1])
    head = shv[...].astype(F32)
    blank = jnp.zeros_like(head)
    head = jnp.concatenate([jnp.where(h == i, head, blank) for i in range(H)], axis=0).T
    sws[...] = head.astype(BF16).reshape(Z, cb, LANES)
    for k in z_order:
        start_copy(sws.at[ring(k)], swr.at[z], one.at[1], at(nz=ring(k)))
    swr[z] = sws[z]
    normed_s = norm_rows(sfv[...], sgv[...].reshape(1, D)).astype(BF16)
    sn[pl.ds(z * C, C)] = normed_s.reshape(C, rows_s // C, D)
    mine = z * C + c
    for k in z_order:
        start_copy(sn.at[mine], sn.at[mine], sn_sems.at[z], at(nz=ring(k), nc=twin))

    wait_sum(loads[2], in_sems.at[2])
    tbt[...] = jnp.broadcast_to(tbv[...], (LANES, L)).T
    sbt[...] = jnp.broadcast_to(sbv[...].reshape(1, L), (LANES, L)).T
    for k in range(D // LANES):
        part = slice(k * LANES, (k + 1) * LANES)
        wt[:, part] = wv[part, :].astype(F32).T.astype(BF16)

    def from_core(group):
        if other:
            wait_bytes(xn.at[pl.ds(0, len(groups[group]) * X)], core_sems.at[group])

    def logits_of(group):
        b = halves[group]
        held = jnp.concatenate(
            [xn[pl.ds(a * half_blocks + b * qb, qb)].reshape(iq, D) for a in range(H)], axis=0
        )
        for part in (slice(0, L // 2), slice(L // 2, L)):
            lg[part, :] = lax.dot_general(wt[part, :], held, NT, preferred_element_type=F32)
        tops, sums = [], []
        for to in range(Z):
            rows = slice(to * cb, (to + 1) * cb)
            part = lg[rows, :] + tbt[rows, 0:1]
            top = jnp.max(part, axis=0, keepdims=True)
            part = part - top
            for a in range(H):
                send[b, a, to] = part[:, a * iq : (a + 1) * iq].astype(BF16)
            for a in range(H):
                bm[to, a, b] = top[:, a * iq : (a + 1) * iq]
            tops.append(top)
            sums.append(jnp.sum(jnp.exp(part), axis=0, keepdims=True))
        for i, a in enumerate((1 - h, h)):
            for k in z_order:
                to = ring(k)
                start_copy(send.at[b, a, to], rb.at[b, a, z], rb_sems.at[2 * group + i], at(nz=to))
        top = functools.reduce(jnp.maximum, tops)
        st[b, me] = top + jnp.log(sum(v * jnp.exp(t - top) for v, t in zip(sums, tops)))
        for ny, nx in plane:
            start_copy(st.at[b, me], st.at[b, me], st_sems.at[group], at(ny=ny, nx=nx, nc=hub))
        to_own_hub(st.at[b, me], st_sems.at[group])

    def pair_head():
        wait_bytes(swr.at[pl.ds(0, Z - 1)], one.at[1])
        for j in range(Z // 2):
            turned = pltpu.roll(swr[j + Z // 2].astype(F32), lane_half, 1)
            swp[j] = (swr[j].astype(F32) + turned).astype(BF16)
        start_copy(swp, swq, one.at[0], at(nh=1 - h))

    for k in list(second) + near:
        arrived(k, x)
        if k in second:
            for px in row_out:
                forward(k, x, at(nx=px, nc=twin))
        to_core(k, x)
    for k in first:
        for px in row_in:
            arrived(k, px)
            to_core(k, px)
    pair_head()
    from_core(0)
    logits_of(0)
    for k in second:
        for px in row_in:
            arrived(k, px)
            to_core(k, px)
    from_core(1)
    logits_of(1)
    member = z * H + h
    for k in z_order + [0]:
        for ph in (1 - h, h):
            if k or ph is not h:
                start_copy(bm.at[ring(k), ph], br.at[member], br_sems.at[0], at(nz=ring(k), nh=ph))
    br[member] = bm[z, h]

    for k in range(1, Z):
        block = ring(k) * C + twin
        wait_bytes(sn.at[block], sn_sems.at[ring(k)])
        for e in other:
            start_copy(sn.at[block], sn.at[block], core_sems.at[2], at(nc=e))
    if other:
        wait_bytes(sn.at[pl.ds(0, Z - 1)], core_sems.at[2])
    wait_bytes(swq, one.at[0])
    lane = lax.broadcasted_iota(jnp.int32, (cb, LANES), 1)
    theirs = jnp.where(lane >= lane_half, 1, 0) != h
    for j in range(Z // 2):
        packed = swq[j].astype(F32)
        turned = pltpu.roll(packed, lane_half, 1)
        for i, value in ((j, packed), (j + Z // 2, turned)):
            swx[i] = jnp.where(theirs, value, swr[i].astype(F32)).astype(BF16)
    scores = jnp.zeros((cb, ih), F32)
    for k in range(Z):
        part = slice(k * LANES, (k + 1) * LANES)
        scores = scores + lax.dot_general(
            swx[k], sn[:, :, part].reshape(ih, LANES), NT, preferred_element_type=F32
        )
    my_rows = pl.ds(pl.multiple_of(z * cb, 16), cb)
    alphas = jnp.exp(scores + sbt[my_rows, 0:1])
    al_s[...] = alphas
    ad[me] = jnp.sum(alphas, axis=0, keepdims=True)
    for ny, nx in plane:
        start_copy(ad.at[me], ad.at[me], one.at[2], at(ny=ny, nx=nx, nc=hub))
    to_own_hub(ad.at[me], one.at[2])

    @pl.when(c == hub)
    def _():
        for group in range(2):
            wait_bytes(st.at[halves[group], pl.ds(0, dpn - 1)], st_sems.at[group])
        tops = st[...]
        top = jnp.max(tops, axis=1)
        log_norm = top + jnp.log(jnp.sum(jnp.exp(tops - top[:, None]), axis=1))
        for a in range(H):
            vs[a] = log_norm[:, :, a * iq : (a + 1) * iq]
        for k in z_order + [0]:
            for ph in (1 - h, h):
                for e in other + [c]:
                    if k or ph is not h or e is not c:
                        start_copy(
                            vs.at[ph], vr.at[member], one.at[3], at(nz=ring(k), nh=ph, nc=e), 1
                        )
        vr[member] = vs[h]

    def summed(group, i):
        b, a = halves[group], (1 - h, h)[i]
        wait_bytes(rb.at[b, a, pl.ds(0, Z - 1)], rb_sems.at[2 * group + i])
        rb[b, a, z] = send[b, a, z]
        return b, jnp.sum(rb[b, a].astype(F32), axis=0)

    def to_partner(group):
        b, total = summed(group, 0)
        tb_s[b] = total.astype(BF16)
        start_copy(tb_s.at[b], tp.at[b], one.at[5], at(nh=1 - h))

    to_partner(0)
    @pl.when(c == hub)
    def _():
        wait_bytes(ad.at[pl.ds(0, dpn - 1)], one.at[2])
        asum[...] = jnp.sum(ad[...], axis=0)
        for k in z_order + [0]:
            for e in other + [c]:
                if k or e is not c:
                    start_copy(asum, az.at[z], one.at[4], at(nz=ring(k), nc=e), 1)
        az[z] = asum[...]

    lgamma, digamma = gamma_parts(al_s[...])
    to_partner(1)
    for group in range(2):
        b, total = summed(group, 1)
        tz[b] = total
    wait_from_hubs(az, Z, one.at[4])
    lgamma_sum, digamma_sum = gamma_parts(jnp.sum(az[...], axis=0))
    wait_bytes(tp, one.at[5])
    wait_bytes(br.at[pl.ds(0, Z * H - 1)], br_sems.at[0])
    shift = jnp.sum(br[...], axis=0)
    wait_from_hubs(vr, Z * H, one.at[3])
    shift = shift - jnp.sum(vr[...], axis=0)
    target = jnp.concatenate(
        [tz[b] + tp[b].astype(F32) + shift[b] for b in range(2)], axis=1
    ) / (Z * H)

    alphas = al_s[...]
    signal = alphas * (digamma - digamma_sum - target)
    high = signal.astype(BF16)
    rest = signal - high.astype(F32)
    mid = rest.astype(BF16)
    low = (rest - mid.astype(F32)).astype(BF16)
    parts = lax.dot_general(
        jnp.concatenate([high, mid, low], axis=0),
        sn[...].reshape(ih, D),
        (((1,), (0,)), ((), ())),
        preferred_element_type=F32,
    )
    grad = parts[:cb] + parts[cb : 2 * cb] + parts[2 * cb :]
    for k in range(Z):
        hs[k] = grad[:, k * LANES : (k + 1) * LANES].astype(BF16)
    for k in z_order:
        start_copy(hs.at[ring(k)], hr.at[z], one.at[7], at(nz=ring(k)))
    hr[z] = hs[z]

    terms = jnp.sum(lgamma - (alphas - 1.0) * target, axis=0, keepdims=True)
    terms = terms - lgamma_sum / (Z * dpn)
    deep = z * C + c
    ld[deep] = jnp.broadcast_to(jnp.sum(terms, axis=1, keepdims=True), (1, LANES))
    for k in z_order:
        start_copy(ld.at[deep], ld.at[deep], one.at[6], at(nz=ring(k), nc=hub))
    to_own_hub(ld.at[deep], one.at[6])

    bc[...] = jnp.zeros_like(bc)
    bc[my_rows, :] = jnp.broadcast_to(jnp.sum(signal, axis=1, keepdims=True), (cb, LANES))
    bg_s[...] = bc[...].T[0:1]
    for k in z_order:
        start_copy(bg_s, bgr.at[z], one.at[8], at(nz=ring(k)))
    bgr[z] = bg_s[...]

    @pl.when(c == hub)
    def _():
        wait_bytes(ld.at[pl.ds(0, Z * C - 1)], one.at[6])
        wide = (h * Y + y) * X + x
        lz[wide] = jnp.sum(ld[...], axis=0)
        for ph in (1 - h, h):
            for k in reversed(range(Y)):
                for px in row_out + [x]:
                    for e in other + [c]:
                        if k or ph is not h or px is not x or e is not c:
                            start_copy(
                                lz.at[wide],
                                lz.at[wide],
                                one.at[9],
                                at(nh=ph, ny=column[k], nx=px, nc=e),
                                1,
                            )

    wait_bytes(hr.at[pl.ds(0, Z - 1)], one.at[7])
    rows = hr[...].astype(F32).reshape(L, LANES).T
    ht[...] = rows.reshape(H, lane_half, L)
    hb[...] = ht[1 - h].astype(BF16)
    start_copy(hb, hp, one.at[10], at(nh=1 - h))
    wait_bytes(bgr.at[pl.ds(0, Z - 1)], one.at[8])
    bh[...] = jnp.sum(bgr[...], axis=0)
    start_copy(bh, bp, one.at[11], at(nh=1 - h))
    wait_bytes(hp, one.at[10])
    hg_o[...] = (ht[h] + hp[...].astype(F32)) / images
    wait_bytes(bp, one.at[11])
    bias_o[...] = ((bh[...] + bp[...]) / images).reshape(L)
    wait_from_hubs(lz, H * Y * X, one.at[9])
    loss_o[...] = jnp.sum(lz[...], axis=0) / (images * (L * dpn))

    wait_sum(sent[0], out_sems.at[0])

    @pl.when(c == hub)
    def _():
        wait_sum(sent[1], out_sems.at[1])

    if C > 1:

        @pl.when(c != hub)
        def _():
            wait_sum(sent[2], out_sems.at[2])


def deliver(hg, bias, loss, hg_o, bias_o, loss_o, sems):
    copies = [
        pltpu.make_async_copy(src, dst, sems.at[i])
        for i, (src, dst) in enumerate([(hg, hg_o), (bias, bias_o), (loss, loss_o)])
    ]
    for copy in copies:
        copy.start()
    for copy in copies:
        copy.wait()


def on_device(sizes, tf, tg, w, tb, sf, sg, sh, sb):
    Z, H, Y, X, C = sizes
    dpn = Y * X * C
    rows_t, D = tf.shape[1:]
    L = w.shape[2]
    cb = L // Z
    ih = rows_t * dpn // H
    iq = ih // 2
    rows_s = sf.shape[0]
    images = ih * H
    assert D == Z * LANES and rows_s * Z == ih and sh.shape[0] * H == LANES

    def v(shape, dtype=F32):
        return pltpu.VMEM(shape, dtype)

    scratch = [
        v((rows_t, D), BF16), v((1, D)), v((D, L), BF16), v((1, L)),
        v((rows_s, D), BF16), v((D,)), v((L,)), v((LANES // H, L), BF16),
        v((dpn, rows_t, D), BF16), v((L, D), BF16), v((L, LANES)), v((L, ih)),
        v((2, H, Z, cb, iq), BF16), v((2, H, Z, cb, iq), BF16), v((2, cb, iq)), v((2, cb, iq), BF16), v((2, cb, iq), BF16),
        v((Z, H, 2, 1, iq)), v((Z * H, 2, 1, iq)), v((2, dpn, 1, ih)), v((H, 2, 1, iq)), v((Z * H, 2, 1, iq)),
        v((Z * C, rows_s // C, D), BF16), v((Z, cb, LANES), BF16), v((Z, cb, LANES), BF16),
        v((Z // 2, cb, LANES), BF16), v((Z // 2, cb, LANES), BF16), v((Z, cb, LANES), BF16),
        v((L, LANES)), v((dpn, 1, ih)), v((1, ih)), v((Z, 1, ih)), v((cb, ih)),
        v((L, LANES)), v((1, L)), v((Z, 1, L)), v((1, L)), v((1, L)),
        v((Z, cb, LANES), BF16), v((Z, cb, LANES), BF16), v((H, LANES // H, L)),
        v((LANES // H, L), BF16), v((LANES // H, L), BF16),
        v((Z * C, 1, LANES)), v((H * Y * X, 1, LANES)),
        v((2**15, LANES), BF16),
        pltpu.SemaphoreType.DMA((3,)), pltpu.SemaphoreType.DMA((Y * X,)), pltpu.SemaphoreType.DMA((3,)),
        pltpu.SemaphoreType.DMA((Z,)), pltpu.SemaphoreType.DMA((4,)), pltpu.SemaphoreType.DMA((2,)), pltpu.SemaphoreType.DMA((1,)),
        pltpu.SemaphoreType.DMA((12,)), pltpu.SemaphoreType.DMA((3,)),
    ]
    vmem = pl.BlockSpec(memory_space=pltpu.VMEM)
    head_grad, bias_grad, loss = pl.pallas_call(
        functools.partial(step_kernel, sizes),
        out_shape=(
            jax.ShapeDtypeStruct((LANES // H, L), F32),
            jax.ShapeDtypeStruct((L,), F32),
            jax.ShapeDtypeStruct((1, LANES), F32),
        ),
        in_specs=[pl.BlockSpec(memory_space=pl.ANY)] * 8,
        out_specs=(vmem, vmem, vmem),
        scratch_shapes=scratch,
        compiler_params=pltpu.CompilerParams(
            collective_id=0, has_side_effects=True, vmem_limit_bytes=48 * 2**20
        ),
    )(*(pltpu.with_memory_space_constraint(a, pltpu.HBM) for a in (tf, tg, w, tb, sf, sg, sh, sb)))
    head_grad, bias_grad, loss = pl.pallas_call(
        deliver,
        out_shape=(
            jax.ShapeDtypeStruct((LANES // H, L), F32),
            jax.ShapeDtypeStruct((L,), F32),
            jax.ShapeDtypeStruct((1, LANES), F32),
        ),
        in_specs=[vmem] * 3,
        out_specs=[pl.BlockSpec(memory_space=pl.ANY)] * 3,
        scratch_shapes=[pltpu.SemaphoreType.DMA((3,))],
        compiler_params=pltpu.CompilerParams(vmem_limit_bytes=2**20),
    )(head_grad, bias_grad, loss)
    return loss[0, 0], head_grad, bias_grad


def solution(mesh, sizes=(8, 2, 4, 4, 2)):
    torus = Mesh(mesh.devices.reshape(sizes), AXES)
    placed = (
        P(MEMBER, DP, None),
        P(MEMBER, None),
        P(MEMBER, None, DP),
        P(MEMBER, DP),
        P(MEMBER, None),
        P(),
        P(MEMBER, DP),
        P(DP),
    )
    return jax.shard_map(
        functools.partial(on_device, sizes),
        mesh=torus,
        in_specs=placed,
        out_specs=(P(), P(MEMBER, DP), P(DP)),
        check_vma=False,
    )
```

```python
import functools
import math

import jax
import jax.numpy as jnp
from jax import lax
from jax.experimental import pallas as pl
from jax.experimental.pallas import tpu as pltpu
from jax.sharding import Mesh
from jax.sharding import PartitionSpec as P

MEMBER = ("member_0", "member_1")
DP = ("dp_0", "dp_1", "dp_2")
AXES = MEMBER + DP
LANES = 128
F32 = jnp.float32
BF16 = jnp.bfloat16
NT = (((1,), (1,)), ((), ()))


def norm_rows(values, gain_row):
    values = values.astype(F32)
    center = values - jnp.mean(values, axis=-1, keepdims=True)
    spread = jnp.mean(center * center, axis=-1, keepdims=True)
    return center * lax.rsqrt(spread + 1e-06) * gain_row


def gamma_parts(x):
    small = x < 8.0
    base = jnp.where(small, x, 1.0)
    product = base
    harmonic = 1.0 / base
    for step in range(1, 8):
        product = product * (base + step)
        harmonic = harmonic + 1.0 / (base + step)
    big = jnp.where(small, x + 8.0, x)
    log_big = jnp.log(big)
    inv = 1.0 / big
    inv2 = inv * inv
    lgamma = (big - 0.5) * log_big - big + 0.9189385332046727
    lgamma = lgamma + inv * (1.0 / 12 - inv2 * (1.0 / 360 - inv2 * (1.0 / 1260)))
    digamma = log_big - 0.5 * inv - inv2 * (1.0 / 12 - inv2 * (1.0 / 120 - inv2 * (1.0 / 252)))
    lgamma = lgamma - jnp.where(small, jnp.log(product), 0.0)
    digamma = digamma - jnp.where(small, harmonic, 0.0)
    return lgamma, digamma


def wait_bytes(ref, sem):
    pltpu.make_async_copy(ref, ref, sem).wait()


def step_kernel(
    sizes,
    tf_h, tg_h, w_h, tb_h, sf_h, sg_h, sh_h, sb_h,
    hg_o, bias_o, loss_o,
    tfv, tgv, wv, tbv, sfv, sgv, sbv, shv,
    xn, wt, tbt, lg, send, rb, tz, tb_s, tp,
    bm, br, st, vs, vr,
    sn, sws, swr, swp, swq, swx, sbt, ad, asum, az, al_s,
    bc, bg_s, bgr, bh, bp, hs, hr, ht, hb, hp,
    ld, lz,
    tally, in_sems, xn_sems, core_sems, rb_sems, st_sems, br_sems, one, out_sems,
):
    Z, H, Y, X, C = sizes
    z, h, y, x, c = (lax.axis_index(a) for a in AXES)
    dpn = Y * X * C
    me = (y * X + x) * C + c
    D = xn.shape[2]
    rows_t = xn.shape[1]
    L = wt.shape[0]
    cb = L // Z
    half_blocks = dpn // H
    ih = half_blocks * rows_t
    qb = half_blocks // 2
    iq = ih // 2
    rows_s = ih // Z
    q = rows_s // rows_t
    images = ih * H
    lane_half = LANES // H

    hub = C - 1
    sent = [[], [], []]

    def start_copy(src, dst, recv_sem, device, kind=0):
        sent[kind].append(math.prod(src.shape) * src.dtype.itemsize)
        pltpu.make_async_remote_copy(
            src_ref=src,
            dst_ref=dst,
            send_sem=out_sems.at[kind],
            recv_sem=recv_sem,
            device_id=device,
            device_id_type=pl.DeviceIdType.MESH,
        ).start()

    def to_own_hub(ref, recv_sem):
        if C > 1:

            @pl.when(c != hub)
            def _():
                start_copy(ref, ref, recv_sem, at(nc=hub), 2)

    def wait_from_hubs(ref, count, sem):
        @pl.when(c == hub)
        def _():
            wait_bytes(ref.at[pl.ds(0, count - 1)], sem)

        if C > 1:

            @pl.when(c != hub)
            def _():
                wait_bytes(ref.at[pl.ds(0, count)], sem)

    def wait_sum(sizes, sem):
        wait_bytes(tally.at[pl.ds(0, sum(sizes) // (2 * LANES))], sem)

    def at(nz=None, nh=None, ny=None, nx=None, nc=None):
        new = (nz, nh, ny, nx, nc)
        return tuple(old if n is None else n for old, n in zip((z, h, y, x, c), new))

    def spot(py, px, pc):
        d = (py * X + px) * C + pc
        m = d // q
        return (m % H) * half_blocks + (m // H) * q + d % q

    def ring(k):
        return lax.rem(z + k, Z)

    z_order = sorted(range(1, Z), key=lambda k: -min(k, Z - k))
    plane = [
        (lax.rem(y + i, Y), lax.rem(x + j, X)) for i in reversed(range(Y)) for j in range(X) if i or j
    ]
    column = [y]
    if Y > 1:
        column.append(y + 1 - 2 * (y % 2))
    for k in range(2, Y):
        column.append((column[k - 2] + 2) % Y)
    groups = [range(0, Y // 2), range(Y // 2, Y)]
    first, second = groups
    halves = [column[group[0]] // (Y // 2) for group in groups]
    near = [k for k in first if k]
    row_out = [lax.rem(x + j, X) for j in (2, 1, 3) if j < X]
    row_in = [lax.rem(x + j, X) for j in (1, 3, 2) if j < X]
    other = [lax.rem(c + e, C) for e in range(1, C)]

    loads = []
    for i, group in enumerate(
        [
            [(tf_h.at[0], tfv), (tg_h, tgv)],
            [(sf_h, sfv), (sg_h, sgv), (sh_h, shv)],
            [(tb_h, tbv), (sb_h, sbv), (w_h.at[0], wv)],
        ]
    ):
        for src, dst in group:
            pltpu.make_async_copy(src, dst, in_sems.at[i]).start()
        loads.append([math.prod(dst.shape) * dst.dtype.itemsize for _, dst in group])
    barrier = pltpu.get_barrier_semaphore()
    peers = [at(ny=column[k]) for k in range(1, Y)] + [at(nx=px) for px in row_out]
    peers += [at(ny=column[k], nx=px) for k in near for px in row_out]
    peers += [at(nc=e) for e in other] + [at(nz=ring(k)) for k in range(1, Z)] + [at(nh=1 - h)]
    for peer in peers:
        pl.semaphore_signal(barrier, 1, device_id=peer, device_id_type=pl.DeviceIdType.MESH)

    own = spot(y, x, c)
    wait_sum(loads[0], in_sems.at[0])
    xn[own] = norm_rows(tfv[...], tgv[...]).astype(BF16)
    pl.semaphore_wait(barrier, len(peers))

    def forward(k, px, device):
        block = spot(column[k], px, c)
        start_copy(xn.at[block], xn.at[block], xn_sems.at[column[k] * X + px], device)

    def arrived(k, px):
        wait_bytes(xn.at[spot(column[k], px, c)], xn_sems.at[column[k] * X + px])

    def to_core(k, px):
        block = spot(column[k], px, c)
        for e in other:
            start_copy(xn.at[block], xn.at[block], core_sems.at[int(k in second)], at(nc=e))

    for k in list(second) + near:
        forward(0, x, at(ny=column[k]))
    for k in [0] + near:
        for px in row_out:
            forward(0, x, at(ny=column[k], nx=px))
    to_core(0, x)
    wait_sum(loads[1], in_sems.at[1])
    head = shv[...].astype(F32)
    blank = jnp.zeros_like(head)
    head = jnp.concatenate([jnp.where(h == i, head, blank) for i in range(H)], axis=0).T
    sws[...] = head.astype(BF16).reshape(Z, cb, LANES)
    for k in z_order:
        start_copy(sws.at[ring(k)], swr.at[z], one.at[1], at(nz=ring(k)))
    swr[z] = sws[z]
    normed_s = norm_rows(sfv[...], sgv[...].reshape(1, D)).astype(BF16)
    sn[pl.ds(z * C, C)] = normed_s.reshape(C, rows_s // C, D)
    mine = z * C + c
    for k in z_order:
        start_copy(sn.at[mine], sn.at[mine], core_sems.at[3], at(nz=ring(k)))

    wait_sum(loads[2], in_sems.at[2])
    tbt[...] = jnp.broadcast_to(tbv[...], (LANES, L)).T
    sbt[...] = jnp.broadcast_to(sbv[...].reshape(1, L), (LANES, L)).T
    for k in range(D // LANES):
        part = slice(k * LANES, (k + 1) * LANES)
        wt[:, part] = wv[part, :].astype(F32).T.astype(BF16)

    def from_core(group):
        if other:
            wait_bytes(xn.at[pl.ds(0, len(groups[group]) * X)], core_sems.at[group])

    def logits_of(group):
        b = halves[group]
        held = jnp.concatenate(
            [xn[pl.ds(a * half_blocks + b * qb, qb)].reshape(iq, D) for a in range(H)], axis=0
        )
        for part in (slice(0, L // 2), slice(L // 2, L)):
            lg[part, :] = lax.dot_general(wt[part, :], held, NT, preferred_element_type=F32)
        tops, sums = [], []
        for to in range(Z):
            rows = slice(to * cb, (to + 1) * cb)
            part = lg[rows, :] + tbt[rows, 0:1]
            top = jnp.max(part, axis=0, keepdims=True)
            part = part - top
            for a in range(H):
                send[b, a, to] = part[:, a * iq : (a + 1) * iq].astype(BF16)
            for a in range(H):
                bm[to, a, b] = top[:, a * iq : (a + 1) * iq]
            tops.append(top)
            sums.append(jnp.sum(jnp.exp(part), axis=0, keepdims=True))
        for i, a in enumerate((1 - h, h)):
            for k in z_order:
                to = ring(k)
                start_copy(send.at[b, a, to], rb.at[b, a, z], rb_sems.at[2 * group + i], at(nz=to))
        top = functools.reduce(jnp.maximum, tops)
        st[b, me] = top + jnp.log(sum(v * jnp.exp(t - top) for v, t in zip(sums, tops)))
        for ny, nx in plane:
            start_copy(st.at[b, me], st.at[b, me], st_sems.at[group], at(ny=ny, nx=nx, nc=hub))
        to_own_hub(st.at[b, me], st_sems.at[group])

    def pair_head():
        wait_bytes(swr.at[pl.ds(0, Z - 1)], one.at[1])
        for j in range(Z // 2):
            turned = pltpu.roll(swr[j + Z // 2].astype(F32), lane_half, 1)
            swp[j] = (swr[j].astype(F32) + turned).astype(BF16)
        start_copy(swp, swq, one.at[0], at(nh=1 - h))

    for k in list(second) + near:
        arrived(k, x)
        if k in second:
            for px in row_out:
                forward(k, x, at(nx=px))
        to_core(k, x)
    for k in first:
        for px in row_in:
            arrived(k, px)
            to_core(k, px)
    pair_head()
    from_core(0)
    logits_of(0)
    for k in second:
        for px in row_in:
            arrived(k, px)
            to_core(k, px)
    from_core(1)
    logits_of(1)
    member = z * H + h
    for k in z_order + [0]:
        for ph in (1 - h, h):
            if k or ph is not h:
                start_copy(bm.at[ring(k), ph], br.at[member], br_sems.at[0], at(nz=ring(k), nh=ph))
    br[member] = bm[z, h]

    wait_bytes(sn.at[pl.ds(0, Z - 1)], core_sems.at[3])
    for k in range(1, Z):
        block = ring(k) * C + c
        for e in other:
            start_copy(sn.at[block], sn.at[block], core_sems.at[2], at(nc=e))
    if other:
        wait_bytes(sn.at[pl.ds(0, Z - 1)], core_sems.at[2])
    wait_bytes(swq, one.at[0])
    lane = lax.broadcasted_iota(jnp.int32, (cb, LANES), 1)
    theirs = jnp.where(lane >= lane_half, 1, 0) != h
    for j in range(Z // 2):
        packed = swq[j].astype(F32)
        turned = pltpu.roll(packed, lane_half, 1)
        for i, value in ((j, packed), (j + Z // 2, turned)):
            swx[i] = jnp.where(theirs, value, swr[i].astype(F32)).astype(BF16)
    scores = jnp.zeros((cb, ih), F32)
    for k in range(Z):
        part = slice(k * LANES, (k + 1) * LANES)
        scores = scores + lax.dot_general(
            swx[k], sn[:, :, part].reshape(ih, LANES), NT, preferred_element_type=F32
        )
    my_rows = pl.ds(pl.multiple_of(z * cb, 16), cb)
    alphas = jnp.exp(scores + sbt[my_rows, 0:1])
    al_s[...] = alphas
    ad[me] = jnp.sum(alphas, axis=0, keepdims=True)
    for ny, nx in plane:
        start_copy(ad.at[me], ad.at[me], one.at[2], at(ny=ny, nx=nx, nc=hub))
    to_own_hub(ad.at[me], one.at[2])

    @pl.when(c == hub)
    def _():
        for group in range(2):
            wait_bytes(st.at[halves[group], pl.ds(0, dpn - 1)], st_sems.at[group])
        tops = st[...]
        top = jnp.max(tops, axis=1)
        log_norm = top + jnp.log(jnp.sum(jnp.exp(tops - top[:, None]), axis=1))
        for a in range(H):
            vs[a] = log_norm[:, :, a * iq : (a + 1) * iq]
        for k in z_order + [0]:
            for ph in (1 - h, h):
                for e in other + [c]:
                    if k or ph is not h or e is not c:
                        start_copy(
                            vs.at[ph], vr.at[member], one.at[3], at(nz=ring(k), nh=ph, nc=e), 1
                        )
        vr[member] = vs[h]

    def summed(group, i):
        b, a = halves[group], (1 - h, h)[i]
        wait_bytes(rb.at[b, a, pl.ds(0, Z - 1)], rb_sems.at[2 * group + i])
        rb[b, a, z] = send[b, a, z]
        return b, jnp.sum(rb[b, a].astype(F32), axis=0)

    def to_partner(group):
        b, total = summed(group, 0)
        tb_s[b] = total.astype(BF16)
        start_copy(tb_s.at[b], tp.at[b], one.at[5], at(nh=1 - h))

    to_partner(0)
    @pl.when(c == hub)
    def _():
        wait_bytes(ad.at[pl.ds(0, dpn - 1)], one.at[2])
        asum[...] = jnp.sum(ad[...], axis=0)
        for k in z_order + [0]:
            for e in other + [c]:
                if k or e is not c:
                    start_copy(asum, az.at[z], one.at[4], at(nz=ring(k), nc=e), 1)
        az[z] = asum[...]

    lgamma, digamma = gamma_parts(al_s[...])
    to_partner(1)
    for group in range(2):
        b, total = summed(group, 1)
        tz[b] = total
    wait_from_hubs(az, Z, one.at[4])
    lgamma_sum, digamma_sum = gamma_parts(jnp.sum(az[...], axis=0))
    wait_bytes(tp, one.at[5])
    wait_bytes(br.at[pl.ds(0, Z * H - 1)], br_sems.at[0])
    shift = jnp.sum(br[...], axis=0)
    wait_from_hubs(vr, Z * H, one.at[3])
    shift = shift - jnp.sum(vr[...], axis=0)
    target = jnp.concatenate(
        [tz[b] + tp[b].astype(F32) + shift[b] for b in range(2)], axis=1
    ) / (Z * H)

    alphas = al_s[...]
    signal = alphas * (digamma - digamma_sum - target)
    high = signal.astype(BF16)
    rest = signal - high.astype(F32)
    mid = rest.astype(BF16)
    low = (rest - mid.astype(F32)).astype(BF16)
    parts = lax.dot_general(
        jnp.concatenate([high, mid, low], axis=0),
        sn[...].reshape(ih, D),
        (((1,), (0,)), ((), ())),
        preferred_element_type=F32,
    )
    grad = parts[:cb] + parts[cb : 2 * cb] + parts[2 * cb :]
    for k in range(Z):
        hs[k] = grad[:, k * LANES : (k + 1) * LANES].astype(BF16)
    for k in z_order:
        start_copy(hs.at[ring(k)], hr.at[z], one.at[7], at(nz=ring(k)))
    hr[z] = hs[z]

    terms = jnp.sum(lgamma - (alphas - 1.0) * target, axis=0, keepdims=True)
    terms = terms - lgamma_sum / (Z * dpn)
    deep = z * C + c
    ld[deep] = jnp.broadcast_to(jnp.sum(terms, axis=1, keepdims=True), (1, LANES))
    for k in z_order:
        start_copy(ld.at[deep], ld.at[deep], one.at[6], at(nz=ring(k), nc=hub))
    to_own_hub(ld.at[deep], one.at[6])

    bc[...] = jnp.zeros_like(bc)
    bc[my_rows, :] = jnp.broadcast_to(jnp.sum(signal, axis=1, keepdims=True), (cb, LANES))
    bg_s[...] = bc[...].T[0:1]
    for k in z_order:
        start_copy(bg_s, bgr.at[z], one.at[8], at(nz=ring(k)))
    bgr[z] = bg_s[...]

    @pl.when(c == hub)
    def _():
        wait_bytes(ld.at[pl.ds(0, Z * C - 1)], one.at[6])
        wide = (h * Y + y) * X + x
        lz[wide] = jnp.sum(ld[...], axis=0)
        for ph in (1 - h, h):
            for k in reversed(range(Y)):
                for px in row_out + [x]:
                    for e in other + [c]:
                        if k or ph is not h or px is not x or e is not c:
                            start_copy(
                                lz.at[wide],
                                lz.at[wide],
                                one.at[9],
                                at(nh=ph, ny=column[k], nx=px, nc=e),
                                1,
                            )

    wait_bytes(hr.at[pl.ds(0, Z - 1)], one.at[7])
    rows = hr[...].astype(F32).reshape(L, LANES).T
    ht[...] = rows.reshape(H, lane_half, L)
    hb[...] = ht[1 - h].astype(BF16)
    start_copy(hb, hp, one.at[10], at(nh=1 - h))
    wait_bytes(bgr.at[pl.ds(0, Z - 1)], one.at[8])
    bh[...] = jnp.sum(bgr[...], axis=0)
    start_copy(bh, bp, one.at[11], at(nh=1 - h))
    wait_bytes(hp, one.at[10])
    hg_o[...] = (ht[h] + hp[...].astype(F32)) / images
    wait_bytes(bp, one.at[11])
    bias_o[...] = ((bh[...] + bp[...]) / images).reshape(L)
    wait_from_hubs(lz, H * Y * X, one.at[9])
    loss_o[...] = jnp.sum(lz[...], axis=0) / (images * (L * dpn))

    wait_sum(sent[0], out_sems.at[0])

    @pl.when(c == hub)
    def _():
        wait_sum(sent[1], out_sems.at[1])

    if C > 1:

        @pl.when(c != hub)
        def _():
            wait_sum(sent[2], out_sems.at[2])


def deliver(hg, bias, loss, hg_o, bias_o, loss_o, sems):
    copies = [
        pltpu.make_async_copy(src, dst, sems.at[i])
        for i, (src, dst) in enumerate([(hg, hg_o), (bias, bias_o), (loss, loss_o)])
    ]
    for copy in copies:
        copy.start()
    for copy in copies:
        copy.wait()


def on_device(sizes, tf, tg, w, tb, sf, sg, sh, sb):
    Z, H, Y, X, C = sizes
    dpn = Y * X * C
    rows_t, D = tf.shape[1:]
    L = w.shape[2]
    cb = L // Z
    ih = rows_t * dpn // H
    iq = ih // 2
    rows_s = sf.shape[0]
    images = ih * H
    assert D == Z * LANES and rows_s * Z == ih and sh.shape[0] * H == LANES

    def v(shape, dtype=F32):
        return pltpu.VMEM(shape, dtype)

    scratch = [
        v((rows_t, D), BF16), v((1, D)), v((D, L), BF16), v((1, L)),
        v((rows_s, D), BF16), v((D,)), v((L,)), v((LANES // H, L), BF16),
        v((dpn, rows_t, D), BF16), v((L, D), BF16), v((L, LANES)), v((L, ih)),
        v((2, H, Z, cb, iq), BF16), v((2, H, Z, cb, iq), BF16), v((2, cb, iq)), v((2, cb, iq), BF16), v((2, cb, iq), BF16),
        v((Z, H, 2, 1, iq)), v((Z * H, 2, 1, iq)), v((2, dpn, 1, ih)), v((H, 2, 1, iq)), v((Z * H, 2, 1, iq)),
        v((Z * C, rows_s // C, D), BF16), v((Z, cb, LANES), BF16), v((Z, cb, LANES), BF16),
        v((Z // 2, cb, LANES), BF16), v((Z // 2, cb, LANES), BF16), v((Z, cb, LANES), BF16),
        v((L, LANES)), v((dpn, 1, ih)), v((1, ih)), v((Z, 1, ih)), v((cb, ih)),
        v((L, LANES)), v((1, L)), v((Z, 1, L)), v((1, L)), v((1, L)),
        v((Z, cb, LANES), BF16), v((Z, cb, LANES), BF16), v((H, LANES // H, L)),
        v((LANES // H, L), BF16), v((LANES // H, L), BF16),
        v((Z * C, 1, LANES)), v((H * Y * X, 1, LANES)),
        v((2**15, LANES), BF16),
        pltpu.SemaphoreType.DMA((3,)), pltpu.SemaphoreType.DMA((Y * X,)), pltpu.SemaphoreType.DMA((4,)),
        pltpu.SemaphoreType.DMA((4,)), pltpu.SemaphoreType.DMA((2,)), pltpu.SemaphoreType.DMA((1,)),
        pltpu.SemaphoreType.DMA((12,)), pltpu.SemaphoreType.DMA((3,)),
    ]
    vmem = pl.BlockSpec(memory_space=pltpu.VMEM)
    head_grad, bias_grad, loss = pl.pallas_call(
        functools.partial(step_kernel, sizes),
        out_shape=(
            jax.ShapeDtypeStruct((LANES // H, L), F32),
            jax.ShapeDtypeStruct((L,), F32),
            jax.ShapeDtypeStruct((1, LANES), F32),
        ),
        in_specs=[pl.BlockSpec(memory_space=pl.ANY)] * 8,
        out_specs=(vmem, vmem, vmem),
        scratch_shapes=scratch,
        compiler_params=pltpu.CompilerParams(
            collective_id=0, has_side_effects=True, vmem_limit_bytes=48 * 2**20
        ),
    )(*(pltpu.with_memory_space_constraint(a, pltpu.HBM) for a in (tf, tg, w, tb, sf, sg, sh, sb)))
    head_grad, bias_grad, loss = pl.pallas_call(
        deliver,
        out_shape=(
            jax.ShapeDtypeStruct((LANES // H, L), F32),
            jax.ShapeDtypeStruct((L,), F32),
            jax.ShapeDtypeStruct((1, LANES), F32),
        ),
        in_specs=[vmem] * 3,
        out_specs=[pl.BlockSpec(memory_space=pl.ANY)] * 3,
        scratch_shapes=[pltpu.SemaphoreType.DMA((3,))],
        compiler_params=pltpu.CompilerParams(vmem_limit_bytes=2**20),
    )(head_grad, bias_grad, loss)
    return loss[0, 0], head_grad, bias_grad


def solution(mesh, sizes=(8, 2, 4, 4, 2)):
    torus = Mesh(mesh.devices.reshape(sizes), AXES)
    placed = (
        P(MEMBER, DP, None),
        P(MEMBER, None),
        P(MEMBER, None, DP),
        P(MEMBER, DP),
        P(MEMBER, None),
        P(),
        P(MEMBER, DP),
        P(DP),
    )
    return jax.shard_map(
        functools.partial(on_device, sizes),
        mesh=torus,
        in_specs=placed,
        out_specs=(P(), P(MEMBER, DP), P(DP)),
        check_vma=False,
    )
```
